1024 devices in a mesh: gx: 8 (over z_hi, core), gy: 16 (over z_lo, y), gz: 8 (over x).
Axes of the slice: x: 8, y: 8, z: 8 (z_hi: 4, z_lo: 2; z = z_hi * 2 + z_lo), core: 2. Of those that a mesh axis runs over, the one named last changes fastest.
Arguments:
- grads: bfloat16 [1024, 4, 1, 32, 3584], P(('gx', 'gy', 'gz')), may hold values from -1196032 to 1196032
- counts: int32 [1024], P(('gx', 'gy', 'gz')), may hold values from 1 to 4
- total_tokens: int32 [1], replicated, may hold values from 4000000 to 15999999
- master: float32 [1, 32, 3584], P(None, 'gy', ('gx', 'gz')), may hold values from -6 to 6
- moment1: float32 [1, 32, 3584], P(None, 'gy', ('gx', 'gz')), may hold values from -2 to 2
- moment2: float32 [1, 32, 3584], P(None, 'gy', ('gx', 'gz')), may hold values from 0.01 to 1
Outputs:
- params: bfloat16 [1, 32, 3584], replicated
- master_out: float32 [1, 32, 3584], P(None, 'gy', ('gx', 'gz'))
- moment1_out: float32 [1, 32, 3584], P(None, 'gy', ('gx', 'gz'))
- moment2_out: float32 [1, 32, 3584], P(None, 'gy', ('gx', 'gz'))
The draws below stay inside these ranges and needn't reach their ends.
All inputs are finite; a program needn't handle non-finite values.
Results may differ from the reference program's by a relative error of at most 0.0004.
Values may be sent and summed in bfloat16 or wider, within the bound.
No kernel may reach another device: no remote copies, remote signals or barrier semaphores. Data moves between devices by JAX's collectives and lax.ppermute only.
A program may use at most 32 MiB of HBM per device.

```python
import math
import jax
import jax.numpy as jnp
from jax import lax

D = 3584
MICRO = 4
BUCKETS = 1
ROWS = 32
DEVICES = 1024


def set_ends(result, stream_key, smallest, largest):
    extent = result.shape
    place = [jax.random.randint(jax.random.fold_in(stream_key, axis), (), 0, extent[axis]) for axis in range(len(extent))]
    result = result.at[tuple(place)].set(smallest)
    longest = extent.index(max(extent))
    place[longest] = (place[longest] + 1) % extent[longest]
    return result.at[tuple(place)].set(largest)


def raised(values, own_key, source, target, blocks, factor):
    owner, partner = [(jnp.arange(values.shape[dim]) // (values.shape[dim] // blocks)).reshape([-1 if axis == dim else 1 for axis in range(values.ndim)]) for dim in (source, target)]
    chosen = jax.random.permutation(own_key, blocks)[partner]
    strong = (owner == chosen) | (owner == (partner + blocks // 2) % blocks)
    return jnp.where(strong, factor * values, values)


def level_of(own_key, dims, split, smallest, top_value):
    def one(position, parts):
        heights = jax.random.uniform(jax.random.fold_in(jax.random.fold_in(own_key, 6), position), (parts,), jnp.float32, smallest / len(split), top_value / len(split))
        return jnp.repeat(jnp.exp(heights), dims[position] // parts).reshape((-1,) + (1,) * (len(dims) - position - 1))

    level = one(*split[0])
    for cut in split[1:]:
        level = level * one(*cut)
    return level


def centred(key, shape, scale, limit, cuts=(), held_as=jnp.bfloat16):
    result = scale * jax.random.normal(key, shape, jnp.float32)
    if cuts:
        result = result * level_of(key, shape, cuts, -0.22, 0.18)
    return jnp.clip(result, -limit, limit).astype(held_as)


def heavy_noise(stream_key, shape, deviation, reach, shards, heavy, held_as=jnp.bfloat16):
    entries = deviation * jax.random.normal(stream_key, shape, jnp.float32)
    if shards:
        entries = entries * level_of(stream_key, shape, shards, -0.22, 0.18)
    return jnp.clip(raised(entries, jax.random.fold_in(stream_key, 3), *heavy), -reach, reach).astype(held_as)


def setup_inputs(seed: int = 0) -> dict:
    keys = jax.random.split(jax.random.key(seed), 7)
    return {
        "grads": heavy_noise(keys[0], (DEVICES, MICRO, BUCKETS, ROWS, D), 200000.0, 1196032, ((0, 1024),), (0, 3, 32, 2.75)),
        "counts": set_ends(jax.random.randint(keys[1], (DEVICES,), 1, 5), jax.random.fold_in(keys[1], 1), 1, 4).astype(jnp.int32),
        "total_tokens": jax.random.randint(keys[2], (1,), 4000000, 16000000).astype(jnp.int32),
        "master": centred(keys[3], (BUCKETS, ROWS, D), 1.0, 6.0, ((1, 16), (2, 64)), jnp.float32),
        "moment1": centred(keys[4], (BUCKETS, ROWS, D), 0.3, 2.0, ((1, 16), (2, 64)), jnp.float32),
        "moment2": jnp.clip(jnp.exp(math.log(1.0) - 4.6051702 * jax.random.uniform(keys[5], (BUCKETS, ROWS, D), jnp.float32) ** level_of(keys[5], (BUCKETS, ROWS, D), ((1, 16), (2, 64)), -0.2, 0.2)), 0.01, 1.0),
    }


def reference(grads, counts, total_tokens, master, moment1, moment2):
    slots = jnp.arange(MICRO, dtype=jnp.int32)

    def add_rank(carry, item):
        rank_grads, rank_count = item
        weights = (slots < rank_count).astype(jnp.float32)
        local = jnp.zeros(carry.shape, jnp.float32)
        for slot in range(MICRO):
            local = local + weights[slot] * rank_grads[slot].astype(jnp.float32)
        return (carry + local, None)
    start = jnp.zeros((BUCKETS, ROWS, D), jnp.float32)
    summed, unused = lax.scan(add_rank, start, (grads, counts))
    gradient = summed / total_tokens.astype(jnp.float32)[0]
    moment1_out = 0.9 * moment1 + 0.1 * gradient
    moment2_out = 0.95 * moment2 + 0.05 * gradient * gradient
    first_fix = 1.0 - 0.9 ** 10
    second_fix = 1.0 - 0.95 ** 10
    update = moment1_out / first_fix / (jnp.sqrt(moment2_out / second_fix) + 1e-08)
    master_out = master - 0.01 * (update + 0.1 * master)
    params = master_out.astype(jnp.bfloat16)
    return (params, master_out, moment1_out, moment2_out)
```

```python
import jax
import jax.numpy as jnp
from jax import lax
from jax.experimental import pallas as pl
from jax.experimental.pallas import tpu as pltpu
from jax.sharding import PartitionSpec as P

COLS = ("gx", "gz")
ROWS = "gy"
VMEM = pl.BlockSpec(memory_space=pltpu.VMEM)
SMEM = pl.BlockSpec(memory_space=pltpu.SMEM)
HBM = pl.BlockSpec(memory_space=pltpu.HBM)
CHUNKS = 4
PARAMS = pltpu.CompilerParams(vmem_limit_bytes=8 * 1024 * 1024)


def accumulate(counts, tokens, grads, master, moment1, moment2, out, state, slots, acc, sems, small):
    _, n_slots, _, rows, width = grads.shape
    peers, half, two_w = out.shape
    w = two_w // 2
    step = width // CHUNKS
    copies = [
        pltpu.make_async_copy(grads.at[0, :, 0, :, pl.ds(c * step, step)], slots.at[:, :, pl.ds(c * step, step)], sems.at[c])
        for c in range(CHUNKS)
    ]
    state_copies = [
        pltpu.make_async_copy(x.at[0], small.at[i], sems.at[CHUNKS + i]) for i, x in enumerate((master, moment1, moment2))
    ]
    for copy in copies:
        copy.start()
    for copy in state_copies:
        copy.start()
    count = counts[0]
    for c in range(CHUNKS):
        copies[c].wait()
        at = slice(c * step, (c + 1) * step)
        total = slots[0, :, at].astype(jnp.float32)
        for slot in range(1, n_slots):
            weight = (slot < count).astype(jnp.float32)
            total = total + weight * slots[slot, :, at].astype(jnp.float32)
        acc[:, at] = total
        for j in range(c * peers // CHUNKS, (c + 1) * peers // CHUNKS):
            out[j, :, :w] = acc[:half, j * w : (j + 1) * w]
            out[j, :, w:] = acc[half:, j * w : (j + 1) * w]
    for copy in state_copies:
        copy.wait()
    state[0:2, :w] = small[0]
    state[0:2, w:] = small[1]
    state[2:4, :w] = small[2]
    state[2:4, w:] = jnp.full((2, w), tokens[0].astype(jnp.float32))
    state[4:8, :] = jnp.zeros((4, two_w), jnp.float32)


def reduce_and_pack(parts, state, out):
    half = parts.shape[1]
    total = parts[0]
    for j in range(1, parts.shape[0]):
        total = total + parts[j]
    for j in range(out.shape[0]):
        out[j, :half, :] = total
        out[j, half:, :] = state[...]


def adam(parts, send, master_out, moment1_out, moment2_out, state, result):
    peers = parts.shape[0]
    half, two_w = send.shape[1:]
    w = two_w // 2
    total = parts[0, :half, :]
    for j in range(1, peers):
        total = total + parts[j, :half, :]
    for j in range(peers):
        h, y = divmod(j, peers // 2)
        at = slice(h * w, (h + 1) * w)
        state[0, 2 * y : 2 * y + 2, at] = parts[j, half : half + 2, :w]
        state[1, 2 * y : 2 * y + 2, at] = parts[j, half : half + 2, w:]
        state[2, 2 * y : 2 * y + 2, at] = parts[j, half + 2 : half + 4, :w]
    master, moment1, moment2 = state[0], state[1], state[2]
    gradient = total / parts[0, half + 2 : half + 3, w : w + 1]
    first = 0.9 * moment1 + 0.1 * gradient
    second = 0.95 * moment2 + 0.05 * gradient * gradient
    first_fix = 1.0 - 0.9**10
    second_fix = 1.0 - 0.95**10
    update = first / first_fix / (jnp.sqrt(second / second_fix) + 1e-08)
    new_master = master - 0.01 * (update + 0.1 * master)
    params = new_master.astype(jnp.bfloat16)
    for j in range(send.shape[0]):
        send[j] = params
    result[0], result[1], result[2] = new_master, first, second
    mine = lax.axis_index(ROWS)
    h, y = mine // (peers // 2), mine % (peers // 2)
    for i, out in enumerate((master_out, moment1_out, moment2_out)):
        rows = result[i, pl.ds(2 * y, 2), :]
        out[0] = jnp.where(h == 0, rows[:, :w], rows[:, w:])


def assemble(parts, out):
    peers, half, two_w = parts.shape
    w = two_w // 2
    for j in range(peers):
        out[0, :half, j * w : (j + 1) * w] = parts[j, :, :w]
        out[0, half:, j * w : (j + 1) * w] = parts[j, :, w:]


def body(grads, counts, total_tokens, master, moment1, moment2):
    f32, bf16 = jnp.float32, jnp.bfloat16
    rows, width = grads.shape[3:]
    n_cols, n_rows = lax.axis_size(COLS), lax.axis_size(ROWS)
    half, two_w = rows // 2, 2 * width // n_cols
    exchange = lambda x, axes: lax.all_to_all(x, axes, 0, 0, tiled=True)

    parts, state = pl.pallas_call(
        accumulate,
        out_shape=(jax.ShapeDtypeStruct((n_cols, half, two_w), f32), jax.ShapeDtypeStruct((8, two_w), f32)),
        in_specs=[SMEM] * 2 + [HBM] * 4,
        out_specs=(VMEM, VMEM),
        scratch_shapes=[
            pltpu.VMEM((grads.shape[1], rows, width), bf16),
            pltpu.VMEM((rows, width), f32),
            pltpu.SemaphoreType.DMA((CHUNKS + 3,)),
            pltpu.VMEM((3, *master.shape[1:]), f32),
        ],
        compiler_params=PARAMS,
    )(counts, total_tokens, *(pltpu.with_memory_space_constraint(x, pltpu.HBM) for x in (grads, master, moment1, moment2)))
    parts = exchange(parts, COLS)
    packed = pl.pallas_call(
        reduce_and_pack,
        out_shape=jax.ShapeDtypeStruct((n_rows, half + 8, two_w), f32),
        in_specs=[VMEM, VMEM],
        out_specs=VMEM,
        compiler_params=PARAMS,
    )(parts, state)
    packed = exchange(packed, ROWS)
    shard = jax.ShapeDtypeStruct(master.shape, f32)
    send, master_out, moment1_out, moment2_out = pl.pallas_call(
        adam,
        out_shape=(jax.ShapeDtypeStruct((n_cols, half, two_w), bf16), shard, shard, shard),
        in_specs=[VMEM],
        out_specs=(VMEM,) * 4,
        scratch_shapes=[pltpu.VMEM((3, half, two_w), f32), pltpu.VMEM((3, half, two_w), f32)],
        compiler_params=PARAMS,
    )(packed)
    gathered = exchange(send, COLS)
    params = pl.pallas_call(
        assemble,
        out_shape=jax.ShapeDtypeStruct((1, rows, width), bf16),
        in_specs=[VMEM],
        out_specs=VMEM,
        compiler_params=PARAMS,
    )(gathered)
    return (params, master_out, moment1_out, moment2_out)


def solution(mesh):
    state = P(None, "gy", ("gx", "gz"))
    return jax.shard_map(
        body,
        mesh=mesh,
        in_specs=(P(("gx", "gy", "gz"), None, None, None, None), P(("gx", "gy", "gz")), P(), state, state, state),
        out_specs=(P(), state, state, state),
        check_vma=False,
    )
```

```python
import jax
import jax.numpy as jnp
from jax import lax
from jax.experimental import pallas as pl
from jax.experimental.pallas import tpu as pltpu
from jax.sharding import Mesh, PartitionSpec as P

PLANE = ("zh", "gy")
LINE = ("core", "gz")
VMEM = pl.BlockSpec(memory_space=pltpu.VMEM)
SMEM = pl.BlockSpec(memory_space=pltpu.SMEM)
HBM = pl.BlockSpec(memory_space=pltpu.HBM)
PARAMS = pltpu.CompilerParams(vmem_limit_bytes=8 * 1024 * 1024)


def accumulate(counts, tokens, grads, master, moment1, moment2, out, state, slots, acc, small, sems):
    _, n_slots, _, rows, width = grads.shape
    peers, _, block = out.shape
    chunks, n_rows = width // block, rows // 2
    copies = [
        pltpu.make_async_copy(grads.at[0, :, 0, :, pl.ds(c * block, block)], slots.at[:, :, pl.ds(c * block, block)], sems.at[c])
        for c in range(chunks)
    ]
    state_copies = [
        pltpu.make_async_copy(x.at[0], small.at[i], sems.at[chunks + i]) for i, x in enumerate((master, moment1, moment2))
    ]
    for copy in copies + state_copies:
        copy.start()
    count = counts[0]
    for c in range(chunks):
        copies[c].wait()
        at = slice(c * block, (c + 1) * block)
        total = slots[0, :, at].astype(jnp.float32)
        for slot in range(1, n_slots):
            weight = (slot < count).astype(jnp.float32)
            total = total + weight * slots[slot, :, at].astype(jnp.float32)
        acc[:, at] = total
        for i in range(n_rows):
            out[c * n_rows + i] = acc[2 * i : 2 * i + 2, at]
    for copy in state_copies:
        copy.wait()
    w = small.shape[-1]
    for i in range(3):
        state[:, i * w : (i + 1) * w] = small[i]
    state[:, 3 * w :] = jnp.full((2, state.shape[1] - 3 * w), tokens[0].astype(jnp.float32))


def reduce_and_pack(parts, state, out):
    block = parts.shape[2]
    total = parts[0]
    for j in range(1, parts.shape[0]):
        total = total + parts[j]
    for j in range(out.shape[0]):
        out[j, :, :block] = total
        out[j, :, block:] = state[...]


def adam(parts, send, master_out, moment1_out, moment2_out, state, result):
    peers = parts.shape[0]
    _, _, block = send.shape
    w = block // peers
    total = parts[0, :, :block]
    for j in range(1, peers):
        total = total + parts[j, :, :block]
    for j in range(peers):
        for i in range(3):
            state[i, :, j * w : (j + 1) * w] = parts[j, :, block + i * w : block + (i + 1) * w]
    master, moment1, moment2 = state[0], state[1], state[2]
    tokens = parts[0, 0:1, block + 3 * w : block + 3 * w + 1]
    gradient = total / tokens
    first = 0.9 * moment1 + 0.1 * gradient
    second = 0.95 * moment2 + 0.05 * gradient * gradient
    first_fix = 1.0 - 0.9**10
    second_fix = 1.0 - 0.95**10
    update = first / first_fix / (jnp.sqrt(second / second_fix) + 1e-08)
    new_master = master - 0.01 * (update + 0.1 * master)
    params = new_master.astype(jnp.bfloat16)
    for j in range(send.shape[0]):
        send[j] = params
    result[0], result[1], result[2] = new_master, first, second
    mine = lax.axis_index(LINE)
    for j in range(peers):

        @pl.when(mine == j)
        def _():
            for i, out in enumerate((master_out, moment1_out, moment2_out)):
                out[0] = result[i, :, j * w : (j + 1) * w]


def assemble(parts, out):
    peers, _, block = parts.shape
    n_rows = out.shape[1] // 2
    for j in range(peers):
        c, i = divmod(j, n_rows)
        out[0, 2 * i : 2 * i + 2, c * block : (c + 1) * block] = parts[j]


def body(grads, counts, total_tokens, master, moment1, moment2):
    f32, bf16 = jnp.float32, jnp.bfloat16
    n_slots, _, rows, width = grads.shape[1:]
    n_plane, n_line = lax.axis_size(PLANE), lax.axis_size(LINE)
    block, w = width // lax.axis_size("zh"), master.shape[2]
    extra = -(-(3 * w + 1) // 128) * 128
    exchange = lambda x, axes: lax.all_to_all(x, axes, 0, 0, tiled=True)
    pinned = [pltpu.with_memory_space_constraint(x, pltpu.HBM) for x in (grads, master, moment1, moment2)]

    parts, state = pl.pallas_call(
        accumulate,
        out_shape=(jax.ShapeDtypeStruct((n_plane, 2, block), f32), jax.ShapeDtypeStruct((2, extra), f32)),
        in_specs=[SMEM] * 2 + [HBM] * 4,
        out_specs=(VMEM, VMEM),
        scratch_shapes=[
            pltpu.VMEM((n_slots, rows, width), bf16),
            pltpu.VMEM((rows, width), f32),
            pltpu.VMEM((3, 2, w), f32),
            pltpu.SemaphoreType.DMA((width // block + 3,)),
        ],
        compiler_params=PARAMS,
    )(counts, total_tokens, *pinned)
    parts = exchange(parts, PLANE)
    packed = pl.pallas_call(
        reduce_and_pack,
        out_shape=jax.ShapeDtypeStruct((n_line, 2, block + extra), f32),
        in_specs=[VMEM, VMEM],
        out_specs=VMEM,
        compiler_params=PARAMS,
    )(parts, state)
    packed = exchange(packed, LINE)
    shard = jax.ShapeDtypeStruct(master.shape, f32)
    send, master_out, moment1_out, moment2_out = pl.pallas_call(
        adam,
        out_shape=(jax.ShapeDtypeStruct((n_plane, 2, block), bf16), shard, shard, shard),
        in_specs=[VMEM],
        out_specs=(VMEM,) * 4,
        scratch_shapes=[pltpu.VMEM((3, 2, block), f32), pltpu.VMEM((3, 2, block), f32)],
        compiler_params=PARAMS,
    )(packed)
    gathered = exchange(send, PLANE)
    params = pl.pallas_call(
        assemble,
        out_shape=jax.ShapeDtypeStruct((1, rows, width), bf16),
        in_specs=[VMEM],
        out_specs=VMEM,
        compiler_params=PARAMS,
    )(gathered)
    return (params, master_out, moment1_out, moment2_out)


def solution(mesh):
    gx, gy, gz = mesh.devices.shape
    fine = Mesh(mesh.devices.reshape(gx // 2, 2, gy, gz), ("zh", "core", "gy", "gz"))
    ranks = ("zh", "core", "gy", "gz")
    state = P(None, "gy", ("zh", "core", "gz"))
    return jax.shard_map(
        body,
        mesh=fine,
        in_specs=(P(ranks, None, None, None, None), P(ranks), P(), state, state, state),
        out_specs=(P(), state, state, state),
        check_vma=False,
    )
```

```python
import functools

import jax
import jax.numpy as jnp
from jax import lax
from jax.experimental import pallas as pl
from jax.experimental.pallas import tpu as pltpu
from jax.sharding import Mesh, PartitionSpec as P

PLANE = ("core", "gy")
LINE = ("zh", "gz")
VMEM = pl.BlockSpec(memory_space=pltpu.VMEM)
SMEM = pl.BlockSpec(memory_space=pltpu.SMEM)
HBM = pl.BlockSpec(memory_space=pltpu.HBM)
PARAMS = pltpu.CompilerParams(vmem_limit_bytes=8 * 1024 * 1024)
F32, BF16 = jnp.float32, jnp.bfloat16


def accumulate(pieces, counts, tokens, grads, master, moment1, moment2, out, state, slots, acc, small, sems):
    _, n_slots, _, rows, width = grads.shape
    peers, _, block = out.shape
    n_rows = rows // 2
    cores, piece = peers // n_rows, block // pieces
    span = piece * cores
    copies = [
        pltpu.make_async_copy(grads.at[0, :, 0, :, pl.ds(z * span, span)], slots.at[:, :, pl.ds(z * span, span)], sems.at[z])
        for z in range(pieces)
    ]
    later = [pltpu.make_async_copy(x.at[0], small.at[i], sems.at[pieces + i]) for i, x in enumerate((master, moment1, moment2))]
    for copy in copies + later:
        copy.start()
    count = counts[0]
    weights = [(slot < count).astype(F32) for slot in range(n_slots)]
    for z in range(pieces):
        copies[z].wait()
        at = slice(z * span, (z + 1) * span)
        total = slots[0, :, at].astype(F32)
        for slot in range(1, n_slots):
            total = total + weights[slot] * slots[slot, :, at].astype(F32)
        for c in range(cores):
            acc[c, :, z * piece : (z + 1) * piece] = total[:, c * piece : (c + 1) * piece]
    for c in range(cores):
        for i in range(n_rows):
            out[c * n_rows + i] = acc[c, 2 * i : 2 * i + 2, :]
    for copy in later:
        copy.wait()
    w = small.shape[-1]
    for i in range(3):
        state[:, i * w : (i + 1) * w] = small[i]
    state[:, 3 * w :] = jnp.full((2, state.shape[1] - 3 * w), tokens[0].astype(F32))


def reduce_and_pack(parts, state, out):
    block = parts.shape[2]
    total = parts[0]
    for j in range(1, parts.shape[0]):
        total = total + parts[j]
    for j in range(out.shape[0]):
        out[j, :, :block] = total
        out[j, :, block:] = state[...]


def adam(parts, send, mine, state, result):
    peers = parts.shape[0]
    _, _, block = send.shape
    w = block // peers
    total = parts[0, :, :block]
    for j in range(1, peers):
        total = total + parts[j, :, :block]
    for j in range(peers):
        for i in range(3):
            state[i, :, j * w : (j + 1) * w] = parts[j, :, block + i * w : block + (i + 1) * w]
    master, moment1, moment2 = state[0], state[1], state[2]
    tokens = parts[0, 0:1, block + 3 * w : block + 3 * w + 1]
    gradient = total / tokens
    first = 0.9 * moment1 + 0.1 * gradient
    second = 0.95 * moment2 + 0.05 * gradient * gradient
    first_fix = 1.0 - 0.9**10
    second_fix = 1.0 - 0.95**10
    update = first / first_fix / (jnp.sqrt(second / second_fix) + 1e-08)
    new_master = master - 0.01 * (update + 0.1 * master)
    params = new_master.astype(BF16)
    for j in range(send.shape[0]):
        send[j] = params
    result[0], result[1], result[2] = new_master, first, second
    place = lax.axis_index(LINE)
    for j in range(peers):

        @pl.when(place == j)
        def _():
            for i in range(3):
                mine[i] = result[i, :, j * w : (j + 1) * w]


def assemble(pieces, parts, mine, params, master_out, moment1_out, moment2_out, whole, sems):
    peers, _, block = parts.shape
    rows, width = whole.shape
    n_rows = rows // 2
    cores, piece = peers // n_rows, block // pieces
    outs = [pltpu.make_async_copy(mine.at[i], x.at[0], sems.at[i]) for i, x in enumerate((master_out, moment1_out, moment2_out))]
    for copy in outs:
        copy.start()
    tile = 8
    for t in range(rows // tile):
        for i in range(t * tile // 2, (t + 1) * tile // 2):
            for c in range(cores):
                for z in range(pieces):
                    start = (z * cores + c) * piece
                    whole[2 * i : 2 * i + 2, start : start + piece] = parts[c * n_rows + i, :, z * piece : (z + 1) * piece]
        at = pl.ds(t * tile, tile)
        copy = pltpu.make_async_copy(whole.at[at], params.at[0, at], sems.at[3 + t])
        copy.start()
        outs.append(copy)
    for copy in outs:
        copy.wait()


def body(grads, counts, total_tokens, master, moment1, moment2):
    n_slots, _, rows, width = grads.shape[1:]
    n_plane, n_line = lax.axis_size(PLANE), lax.axis_size(LINE)
    block, w = rows * width // (2 * n_plane), master.shape[2]
    extra = -(-(3 * w + 1) // 128) * 128
    exchange = lambda x, axes: lax.all_to_all(x, axes, 0, 0, tiled=True)
    pieces = lax.axis_size("zh")
    pinned = [pltpu.with_memory_space_constraint(x, pltpu.HBM) for x in (grads, master, moment1, moment2)]

    parts, state = pl.pallas_call(
        functools.partial(accumulate, pieces),
        out_shape=(jax.ShapeDtypeStruct((n_plane, 2, block), F32), jax.ShapeDtypeStruct((2, extra), F32)),
        in_specs=[SMEM] * 2 + [HBM] * 4,
        out_specs=(VMEM, VMEM),
        scratch_shapes=[
            pltpu.VMEM((n_slots, rows, width), BF16),
            pltpu.VMEM((n_plane * 2 // rows, rows, block), F32),
            pltpu.VMEM((3, 2, w), F32),
            pltpu.SemaphoreType.DMA((pieces + 3,)),
        ],
        compiler_params=PARAMS,
    )(counts, total_tokens, *pinned)
    parts = exchange(parts, PLANE)
    packed = pl.pallas_call(
        reduce_and_pack,
        out_shape=jax.ShapeDtypeStruct((n_line, 2, block + extra), F32),
        in_specs=[VMEM, VMEM],
        out_specs=VMEM,
        compiler_params=PARAMS,
    )(parts, state)
    packed = exchange(packed, LINE)
    send, mine = pl.pallas_call(
        adam,
        out_shape=(jax.ShapeDtypeStruct((n_plane, 2, block), BF16), jax.ShapeDtypeStruct((3, 2, w), F32)),
        in_specs=[VMEM],
        out_specs=(VMEM, VMEM),
        scratch_shapes=[pltpu.VMEM((3, 2, block), F32), pltpu.VMEM((3, 2, block), F32)],
        compiler_params=PARAMS,
    )(packed)
    gathered = exchange(send, PLANE)
    shard = jax.ShapeDtypeStruct(master.shape, F32)
    return pl.pallas_call(
        functools.partial(assemble, pieces),
        out_shape=(jax.ShapeDtypeStruct((1, rows, width), BF16), shard, shard, shard),
        in_specs=[VMEM, VMEM],
        out_specs=(HBM,) * 4,
        scratch_shapes=[pltpu.VMEM((rows, width), BF16), pltpu.SemaphoreType.DMA((3 + rows // 8,))],
        compiler_params=PARAMS,
    )(gathered, mine)


def solution(mesh):
    gx, gy, gz = mesh.devices.shape
    fine = Mesh(mesh.devices.reshape(gx // 2, 2, gy, gz), ("zh", "core", "gy", "gz"))
    ranks = ("zh", "core", "gy", "gz")
    state = P(None, "gy", ("zh", "core", "gz"))
    return jax.shard_map(
        body,
        mesh=fine,
        in_specs=(P(ranks, None, None, None, None), P(ranks), P(), state, state, state),
        out_specs=(P(), state, state, state),
        check_vma=False,
    )
```

```python
import jax
import jax.numpy as jnp
from jax import lax
from jax.experimental import pallas as pl
from jax.experimental.pallas import tpu as pltpu
from jax.sharding import Mesh, PartitionSpec as P

PLANE = ("gy", "zh")
LINE = ("core", "gz")
VMEM = pl.BlockSpec(memory_space=pltpu.VMEM)
SMEM = pl.BlockSpec(memory_space=pltpu.SMEM)
HBM = pl.BlockSpec(memory_space=pltpu.HBM)
PARAMS = pltpu.CompilerParams(vmem_limit_bytes=8 * 1024 * 1024)
F32, BF16 = jnp.float32, jnp.bfloat16


def accumulate(counts, tokens, grads, master, moment1, moment2, out, state, slots, acc, small, sems):
    _, n_slots, _, rows, width = grads.shape
    _, _, block = out.shape
    spans = width // block
    copies = [
        pltpu.make_async_copy(grads.at[0, :, 0, :, pl.ds(z * block, block)], slots.at[:, :, pl.ds(z * block, block)], sems.at[z])
        for z in range(spans)
    ]
    later = [pltpu.make_async_copy(x.at[0], small.at[i], sems.at[spans + i]) for i, x in enumerate((master, moment1, moment2))]
    for copy in copies + later:
        copy.start()
    count = counts[0]
    weights = [(slot < count).astype(F32) for slot in range(n_slots)]
    for z in range(spans):
        copies[z].wait()
        at = slice(z * block, (z + 1) * block)
        total = slots[0, :, at].astype(F32)
        for slot in range(1, n_slots):
            total = total + weights[slot] * slots[slot, :, at].astype(F32)
        acc[:, at] = total
        for i in range(rows // 2):
            out[i * spans + z] = acc[2 * i : 2 * i + 2, at]
    for copy in later:
        copy.wait()
    w = small.shape[-1]
    for i in range(3):
        state[:, i * w : (i + 1) * w] = small[i]
    state[:, 3 * w :] = jnp.full((2, state.shape[1] - 3 * w), tokens[0].astype(F32))


def reduce_and_pack(parts, state, out):
    block = parts.shape[2]
    total = parts[0]
    for j in range(1, parts.shape[0]):
        total = total + parts[j]
    for j in range(out.shape[0]):
        out[j, :, :block] = total
        out[j, :, block:] = state[...]


def adam(parts, send, mine, state, result):
    peers = parts.shape[0]
    _, _, block = send.shape
    w = block // peers
    total = parts[0, :, :block]
    for j in range(1, peers):
        total = total + parts[j, :, :block]
    for j in range(peers):
        for i in range(3):
            state[i, :, j * w : (j + 1) * w] = parts[j, :, block + i * w : block + (i + 1) * w]
    master, moment1, moment2 = state[0], state[1], state[2]
    tokens = parts[0, 0:1, block + 3 * w : block + 3 * w + 1]
    gradient = total / tokens
    first = 0.9 * moment1 + 0.1 * gradient
    second = 0.95 * moment2 + 0.05 * gradient * gradient
    first_fix = 1.0 - 0.9**10
    second_fix = 1.0 - 0.95**10
    update = first / first_fix / (jnp.sqrt(second / second_fix) + 1e-08)
    new_master = master - 0.01 * (update + 0.1 * master)
    params = new_master.astype(BF16)
    for j in range(send.shape[0]):
        send[j] = params
    result[0], result[1], result[2] = new_master, first, second
    place = lax.axis_index(LINE)
    for j in range(peers):

        @pl.when(place == j)
        def _():
            for i in range(3):
                mine[i] = result[i, :, j * w : (j + 1) * w]


def assemble(parts, mine, params, master_out, moment1_out, moment2_out, whole, sems):
    _, _, block = parts.shape
    rows, width = whole.shape
    spans = width // block
    outs = [pltpu.make_async_copy(mine.at[i], x.at[0], sems.at[i]) for i, x in enumerate((master_out, moment1_out, moment2_out))]
    for copy in outs:
        copy.start()
    for t in range(rows // 8):
        for i in range(4 * t, 4 * t + 4):
            for z in range(spans):
                whole[2 * i : 2 * i + 2, z * block : (z + 1) * block] = parts[i * spans + z]
        at = pl.ds(8 * t, 8)
        copy = pltpu.make_async_copy(whole.at[at], params.at[0, at], sems.at[3 + t])
        copy.start()
        outs.append(copy)
    for copy in outs:
        copy.wait()


def body(grads, counts, total_tokens, master, moment1, moment2):
    n_slots, _, rows, width = grads.shape[1:]
    n_plane, n_line = lax.axis_size(PLANE), lax.axis_size(LINE)
    block, w = rows * width // (2 * n_plane), master.shape[2]
    extra = -(-(3 * w + 1) // 128) * 128
    exchange = lambda x, axes: lax.all_to_all(x, axes, 0, 0, tiled=True)
    pinned = [pltpu.with_memory_space_constraint(x, pltpu.HBM) for x in (grads, master, moment1, moment2)]

    parts, state = pl.pallas_call(
        accumulate,
        out_shape=(jax.ShapeDtypeStruct((n_plane, 2, block), F32), jax.ShapeDtypeStruct((2, extra), F32)),
        in_specs=[SMEM] * 2 + [HBM] * 4,
        out_specs=(VMEM, VMEM),
        scratch_shapes=[
            pltpu.VMEM((n_slots, rows, width), BF16),
            pltpu.VMEM((rows, width), F32),
            pltpu.VMEM((3, 2, w), F32),
            pltpu.SemaphoreType.DMA((width // block + 3,)),
        ],
        compiler_params=PARAMS,
    )(counts, total_tokens, *pinned)
    parts = exchange(parts, PLANE)
    packed = pl.pallas_call(
        reduce_and_pack,
        out_shape=jax.ShapeDtypeStruct((n_line, 2, block + extra), F32),
        in_specs=[VMEM, VMEM],
        out_specs=VMEM,
        compiler_params=PARAMS,
    )(parts, state)
    packed = exchange(packed, LINE)
    send, mine = pl.pallas_call(
        adam,
        out_shape=(jax.ShapeDtypeStruct((n_plane, 2, block), BF16), jax.ShapeDtypeStruct((3, 2, w), F32)),
        in_specs=[VMEM],
        out_specs=(VMEM, VMEM),
        scratch_shapes=[pltpu.VMEM((3, 2, block), F32), pltpu.VMEM((3, 2, block), F32)],
        compiler_params=PARAMS,
    )(packed)
    gathered = exchange(send, PLANE)
    shard = jax.ShapeDtypeStruct(master.shape, F32)
    return pl.pallas_call(
        assemble,
        out_shape=(jax.ShapeDtypeStruct((1, rows, width), BF16), shard, shard, shard),
        in_specs=[VMEM, VMEM],
        out_specs=(HBM,) * 4,
        scratch_shapes=[pltpu.VMEM((rows, width), BF16), pltpu.SemaphoreType.DMA((3 + rows // 8,))],
        compiler_params=PARAMS,
    )(gathered, mine)


def solution(mesh):
    gx, gy, gz = mesh.devices.shape
    fine = Mesh(mesh.devices.reshape(gx // 2, 2, gy, gz), ("zh", "core", "gy", "gz"))
    ranks = ("zh", "core", "gy", "gz")
    state = P(None, "gy", ("zh", "core", "gz"))
    return jax.shard_map(
        body,
        mesh=fine,
        in_specs=(P(ranks, None, None, None, None), P(ranks), P(), state, state, state),
        out_specs=(P(), state, state, state),
        check_vma=False,
    )
```

```python
import jax
import jax.numpy as jnp
from jax import lax
from jax.experimental import pallas as pl
from jax.experimental.pallas import tpu as pltpu
from jax.sharding import Mesh, PartitionSpec as P

PLANE = ("gy", "zh")
LINE = ("core", "gz")
VMEM = pl.BlockSpec(memory_space=pltpu.VMEM)
SMEM = pl.BlockSpec(memory_space=pltpu.SMEM)
HBM = pl.BlockSpec(memory_space=pltpu.HBM)
PARAMS = pltpu.CompilerParams(vmem_limit_bytes=8 * 1024 * 1024)
F32, BF16 = jnp.float32, jnp.bfloat16


def accumulate(counts, grads, master, moment1, moment2, keep, give, state, slots, acc, small, sems):
    _, n_slots, _, rows, width = grads.shape
    half = keep.shape[2]
    spans, span = width // (2 * half), 2 * half
    copies = [
        pltpu.make_async_copy(grads.at[0, :, 0, :, pl.ds(z * span, span)], slots.at[:, :, pl.ds(z * span, span)], sems.at[z])
        for z in range(spans)
    ]
    later = [pltpu.make_async_copy(x.at[0], small.at[i], sems.at[spans + i]) for i, x in enumerate((master, moment1, moment2))]
    for copy in copies + later:
        copy.start()
    core = lax.axis_index("core")
    count = counts[0]
    weights = [(slot < count).astype(F32) for slot in range(n_slots)]
    for z in range(spans):
        copies[z].wait()
        at = slice(z * span, (z + 1) * span)
        total = slots[0, :, at].astype(F32)
        for slot in range(1, n_slots):
            total = total + weights[slot] * slots[slot, :, at].astype(F32)
        acc[0, :, z * half : (z + 1) * half] = total[:, :half]
        acc[1, :, z * half : (z + 1) * half] = total[:, half:]
    for own in range(2):

        @pl.when(core == own)
        def _():
            for c, out in ((own, keep), (1 - own, give)):
                for i in range(rows // 2):
                    for z in range(spans):
                        out[i * spans + z] = acc[c, 2 * i : 2 * i + 2, z * half : (z + 1) * half]

    for copy in later:
        copy.wait()
    w = small.shape[-1]
    for i in range(3):
        state[:, i * w : (i + 1) * w] = small[i]


def add(tokens, x, y, shards, out, state):
    used, extra = shards.shape[1], state.shape[1]
    out[...] = x[...] + y[...]
    state[:, :used] = shards[...]
    state[:, used:] = jnp.full((2, extra - used), tokens[0].astype(F32))


def reduce_and_pack(parts, state, out):
    half = parts.shape[2]
    extra = out.shape[2] - half
    total = parts[0]
    for j in range(1, parts.shape[0]):
        total = total + parts[j]
    for j in range(out.shape[0]):
        out[j, :, :half] = total
        out[j, :, half:] = state[:, :extra]


def adam(parts, send, mine, summed, state, result):
    peers = parts.shape[0]
    _, _, block = send.shape
    w, half = block // peers, block // 2
    for c in range(2):
        total = parts[c * peers // 2, :, :half]
        for j in range(c * peers // 2 + 1, (c + 1) * peers // 2):
            total = total + parts[j, :, :half]
        summed[:, c * half : (c + 1) * half] = total
    total = summed[...]
    for j in range(peers):
        for i in range(3):
            state[i, :, j * w : (j + 1) * w] = parts[j, :, half + i * w : half + (i + 1) * w]
    master, moment1, moment2 = state[0], state[1], state[2]
    tokens = parts[0, 0:1, half + 3 * w : half + 3 * w + 1]
    gradient = total / tokens
    first = 0.9 * moment1 + 0.1 * gradient
    second = 0.95 * moment2 + 0.05 * gradient * gradient
    first_fix = 1.0 - 0.9**10
    second_fix = 1.0 - 0.95**10
    update = first / first_fix / (jnp.sqrt(second / second_fix) + 1e-08)
    new_master = master - 0.01 * (update + 0.1 * master)
    params = new_master.astype(BF16)
    for j in range(send.shape[0]):
        send[j] = params
    result[0], result[1], result[2] = new_master, first, second
    place = lax.axis_index(LINE)
    for j in range(peers):

        @pl.when(place == j)
        def _():
            for i in range(3):
                mine[i] = result[i, :, j * w : (j + 1) * w]


def assemble(parts, mine, params, master_out, moment1_out, moment2_out, whole, sems):
    _, _, block = parts.shape
    rows, width = whole.shape
    spans = width // block
    outs = [pltpu.make_async_copy(mine.at[i], x.at[0], sems.at[i]) for i, x in enumerate((master_out, moment1_out, moment2_out))]
    for copy in outs:
        copy.start()
    for t in range(rows // 8):
        for i in range(4 * t, 4 * t + 4):
            for z in range(spans):
                whole[2 * i : 2 * i + 2, z * block : (z + 1) * block] = parts[i * spans + z]
        at = pl.ds(8 * t, 8)
        copy = pltpu.make_async_copy(whole.at[at], params.at[0, at], sems.at[3 + t])
        copy.start()
        outs.append(copy)
    for copy in outs:
        copy.wait()


def body(grads, counts, total_tokens, master, moment1, moment2):
    n_slots, _, rows, width = grads.shape[1:]
    n_plane, n_line = lax.axis_size(PLANE), lax.axis_size(LINE)
    block, w = rows * width // (2 * n_plane), master.shape[2]
    half = block // 2
    whole = -(-(half + 3 * w + 1) // 128) * 128
    exchange = lambda x, axes: lax.all_to_all(x, axes, 0, 0, tiled=True)
    pinned = [pltpu.with_memory_space_constraint(x, pltpu.HBM) for x in (grads, master, moment1, moment2)]

    piece = jax.ShapeDtypeStruct((n_plane, 2, half), F32)
    keep, give, shards = pl.pallas_call(
        accumulate,
        out_shape=(piece, piece, jax.ShapeDtypeStruct((2, 3 * w), F32)),
        in_specs=[SMEM] + [HBM] * 4,
        out_specs=(VMEM,) * 3,
        scratch_shapes=[
            pltpu.VMEM((n_slots, rows, width), BF16),
            pltpu.VMEM((2, rows, width // 2), F32),
            pltpu.VMEM((3, 2, w), F32),
            pltpu.SemaphoreType.DMA((width // block + 3,)),
        ],
        compiler_params=PARAMS,
    )(counts, *pinned)
    given = lax.ppermute(give, "core", [(0, 1), (1, 0)])
    parts, state = pl.pallas_call(
        add,
        out_shape=(piece, jax.ShapeDtypeStruct((2, whole - half), F32)),
        in_specs=[SMEM] + [VMEM] * 3,
        out_specs=(VMEM, VMEM),
        compiler_params=PARAMS,
    )(total_tokens, keep, given, shards)
    parts = exchange(parts, PLANE)
    packed = pl.pallas_call(
        reduce_and_pack,
        out_shape=jax.ShapeDtypeStruct((n_line, 2, whole), F32),
        in_specs=[VMEM, VMEM],
        out_specs=VMEM,
        compiler_params=PARAMS,
    )(parts, state)
    packed = exchange(packed, LINE)
    send, mine = pl.pallas_call(
        adam,
        out_shape=(jax.ShapeDtypeStruct((n_plane, 2, block), BF16), jax.ShapeDtypeStruct((3, 2, w), F32)),
        in_specs=[VMEM],
        out_specs=(VMEM, VMEM),
        scratch_shapes=[pltpu.VMEM((2, block), F32), pltpu.VMEM((3, 2, block), F32), pltpu.VMEM((3, 2, block), F32)],
        compiler_params=PARAMS,
    )(packed)
    gathered = exchange(send, PLANE)
    shard = jax.ShapeDtypeStruct(master.shape, F32)
    return pl.pallas_call(
        assemble,
        out_shape=(jax.ShapeDtypeStruct((1, rows, width), BF16), shard, shard, shard),
        in_specs=[VMEM, VMEM],
        out_specs=(HBM,) * 4,
        scratch_shapes=[pltpu.VMEM((rows, width), BF16), pltpu.SemaphoreType.DMA((3 + rows // 8,))],
        compiler_params=PARAMS,
    )(gathered, mine)


def solution(mesh):
    gx, gy, gz = mesh.devices.shape
    fine = Mesh(mesh.devices.reshape(gx // 2, 2, gy, gz), ("zh", "core", "gy", "gz"))
    ranks = ("zh", "core", "gy", "gz")
    state = P(None, "gy", ("zh", "core", "gz"))
    return jax.shard_map(
        body,
        mesh=fine,
        in_specs=(P(ranks, None, None, None, None), P(ranks), P(), state, state, state),
        out_specs=(P(), state, state, state),
        check_vma=False,
    )
```

```python
import jax
import jax.numpy as jnp
from jax import lax
from jax.experimental import pallas as pl
from jax.experimental.pallas import tpu as pltpu
from jax.sharding import Mesh, PartitionSpec as P

PLANE = ("gy", "zh")
LINE = ("core", "gz")
VMEM = pl.BlockSpec(memory_space=pltpu.VMEM)
SMEM = pl.BlockSpec(memory_space=pltpu.SMEM)
HBM = pl.BlockSpec(memory_space=pltpu.HBM)
PARAMS = pltpu.CompilerParams(vmem_limit_bytes=8 * 1024 * 1024)
LANES, TILE, PAIRS = 128, 8, 6
F32, BF16 = jnp.float32, jnp.bfloat16


def accumulate(counts, grads, master, moment1, moment2, keep, give, shards, slots, acc, small, sems):
    _, n_slots, _, rows, width = grads.shape
    spans = 2 * keep.shape[0] // (TILE * rows)
    span, lines = width // spans, width // (spans * LANES)
    copies = [
        pltpu.make_async_copy(grads.at[0, :, 0, :, pl.ds(z * span, span)], slots.at[:, :, pl.ds(z * span, span)], sems.at[z])
        for z in range(spans)
    ]
    later = [pltpu.make_async_copy(x.at[0], small.at[i], sems.at[spans + i]) for i, x in enumerate((master, moment1, moment2))]
    for copy in copies + later:
        copy.start()
    core = lax.axis_index("core")
    count = counts[0]
    weights = [(slot < count).astype(F32) for slot in range(n_slots)]
    group = min(TILE, rows // 2)
    for z in range(spans):
        copies[z].wait()
        at = slice(z * span, (z + 1) * span)
        total = slots[0, :, at].astype(F32)
        for slot in range(1, n_slots):
            total = total + weights[slot] * slots[slot, :, at].astype(F32)
        for k in range(lines):
            acc[z * lines + k] = total[:, k * LANES : (k + 1) * LANES]
        for k in range(lines):
            for i in range(0, rows // 2, group):
                to = pl.ds((i * spans + z) * TILE + k, group, stride=spans * TILE)
                keep[to, :] = acc[z * lines + k, pl.ds(2 * i + core, group, stride=2), :]
                give[to, :] = acc[z * lines + k, pl.ds(2 * i + 1 - core, group, stride=2), :]
    for copy in later:
        copy.wait()
    w = small.shape[-1]
    shards[...] = jnp.zeros(shards.shape, F32)
    shards[0, :, :w] = small[0]
    shards[0, :, w : 2 * w] = small[1]
    shards[1, :, :w] = small[2]


def add(tokens, x, y, shards, out, state):
    out[...] = x[...] + y[...]
    state[...] = shards[...]
    state[1, :, LANES - 1 :] = jnp.full((2, 1), tokens[0].astype(F32))


def reduce_and_pack(parts, state, out):
    total = parts[0:TILE, :]
    for j in range(TILE, parts.shape[0], TILE):
        total = total + parts[j : j + TILE, :]
    for j in range(0, out.shape[0], PAIRS):
        for r in range(PAIRS - 2):
            out[j + r] = total[2 * r : 2 * r + 2, :]
        out[j + PAIRS - 2] = state[0]
        out[j + PAIRS - 1] = state[1]


def adam(parts, send, mine, summed, state, result):
    peers = parts.shape[0] // PAIRS
    _, _, block = send.shape
    w = block // peers
    for c in range(2):
        for r in range(-(-block // (2 * LANES))):
            first = c * peers // 2
            total = parts[first * PAIRS + r]
            for j in range(first + 1, first + peers // 2):
                total = total + parts[j * PAIRS + r]
            for k in range(2 * r, min(2 * r + 2, block // LANES)):
                summed[c : c + 1, k * LANES : (k + 1) * LANES] = total[k - 2 * r : k - 2 * r + 1, :]
    total = summed[...]
    for j in range(peers):
        at = slice(j * w, (j + 1) * w)
        state[0, :, at] = parts[j * PAIRS + PAIRS - 2, :, :w]
        state[1, :, at] = parts[j * PAIRS + PAIRS - 2, :, w : 2 * w]
        state[2, :, at] = parts[j * PAIRS + PAIRS - 1, :, :w]
    master, moment1, moment2 = state[0], state[1], state[2]
    tokens = parts[PAIRS - 1, 0:1, LANES - 1 :]
    gradient = total / tokens
    first = 0.9 * moment1 + 0.1 * gradient
    second = 0.95 * moment2 + 0.05 * gradient * gradient
    first_fix = 1.0 - 0.9**10
    second_fix = 1.0 - 0.95**10
    update = first / first_fix / (jnp.sqrt(second / second_fix) + 1e-08)
    new_master = master - 0.01 * (update + 0.1 * master)
    params = new_master.astype(BF16)
    for j in range(send.shape[0]):
        send[j] = params
    result[0], result[1], result[2] = new_master, first, second
    place = lax.axis_index(LINE)
    for j in range(peers):

        @pl.when(place == j)
        def _():
            for i in range(3):
                mine[i] = result[i, :, j * w : (j + 1) * w]


def assemble(parts, mine, params, master_out, moment1_out, moment2_out, whole, sems):
    _, _, block = parts.shape
    rows, width = whole.shape
    spans = width // block
    outs = [pltpu.make_async_copy(mine.at[i], x.at[0], sems.at[i]) for i, x in enumerate((master_out, moment1_out, moment2_out))]
    for copy in outs:
        copy.start()
    for t in range(rows // 8):
        for i in range(4 * t, 4 * t + 4):
            for z in range(spans):
                whole[2 * i : 2 * i + 2, z * block : (z + 1) * block] = parts[i * spans + z]
        at = pl.ds(8 * t, 8)
        copy = pltpu.make_async_copy(whole.at[at], params.at[0, at], sems.at[3 + t])
        copy.start()
        outs.append(copy)
    for copy in outs:
        copy.wait()


def body(grads, counts, total_tokens, master, moment1, moment2):
    n_slots, _, rows, width = grads.shape[1:]
    n_plane, n_line = lax.axis_size(PLANE), lax.axis_size(LINE)
    block, w = rows * width // (2 * n_plane), master.shape[2]
    exchange = lambda x, axes: lax.all_to_all(x, axes, 0, 0, tiled=True)
    pinned = [pltpu.with_memory_space_constraint(x, pltpu.HBM) for x in (grads, master, moment1, moment2)]

    tiles = jax.ShapeDtypeStruct((n_plane * TILE, LANES), F32)
    pairs = jax.ShapeDtypeStruct((2, 2, LANES), F32)
    keep, give, shards = pl.pallas_call(
        accumulate,
        out_shape=(tiles, tiles, pairs),
        in_specs=[SMEM] + [HBM] * 4,
        out_specs=(VMEM,) * 3,
        scratch_shapes=[
            pltpu.VMEM((n_slots, rows, width), BF16),
            pltpu.VMEM((width // LANES, rows, LANES), F32),
            pltpu.VMEM((3, 2, w), F32),
            pltpu.SemaphoreType.DMA((width // block + 3,)),
        ],
        compiler_params=PARAMS,
    )(counts, *pinned)
    given = lax.ppermute(give, "core", [(0, 1), (1, 0)])
    parts, state = pl.pallas_call(
        add,
        out_shape=(tiles, pairs),
        in_specs=[SMEM] + [VMEM] * 3,
        out_specs=(VMEM, VMEM),
        compiler_params=PARAMS,
    )(total_tokens, keep, given, shards)
    parts = exchange(parts, PLANE)
    packed = pl.pallas_call(
        reduce_and_pack,
        out_shape=jax.ShapeDtypeStruct((n_line * PAIRS, 2, LANES), F32),
        in_specs=[VMEM, VMEM],
        out_specs=VMEM,
        compiler_params=PARAMS,
    )(parts, state)
    packed = exchange(packed, LINE)
    send, mine = pl.pallas_call(
        adam,
        out_shape=(jax.ShapeDtypeStruct((n_plane, 2, block), BF16), jax.ShapeDtypeStruct((3, 2, w), F32)),
        in_specs=[VMEM],
        out_specs=(VMEM, VMEM),
        scratch_shapes=[pltpu.VMEM((2, block), F32), pltpu.VMEM((3, 2, block), F32), pltpu.VMEM((3, 2, block), F32)],
        compiler_params=PARAMS,
    )(packed)
    gathered = exchange(send, PLANE)
    shard = jax.ShapeDtypeStruct(master.shape, F32)
    return pl.pallas_call(
        assemble,
        out_shape=(jax.ShapeDtypeStruct((1, rows, width), BF16), shard, shard, shard),
        in_specs=[VMEM, VMEM],
        out_specs=(HBM,) * 4,
        scratch_shapes=[pltpu.VMEM((rows, width), BF16), pltpu.SemaphoreType.DMA((3 + rows // 8,))],
        compiler_params=PARAMS,
    )(gathered, mine)


def solution(mesh):
    gx, gy, gz = mesh.devices.shape
    fine = Mesh(mesh.devices.reshape(gx // 2, 2, gy, gz), ("zh", "core", "gy", "gz"))
    ranks = ("zh", "core", "gy", "gz")
    state = P(None, "gy", ("zh", "core", "gz"))
    return jax.shard_map(
        body,
        mesh=fine,
        in_specs=(P(ranks, None, None, None, None), P(ranks), P(), state, state, state),
        out_specs=(P(), state, state, state),
        check_vma=False,
    )
```

```python
import jax
import jax.numpy as jnp
from jax import lax
from jax.experimental import pallas as pl
from jax.experimental.pallas import tpu as pltpu
from jax.sharding import Mesh, PartitionSpec as P

PLANE = ("gy", "zh")
LINE = ("core", "gz")
VMEM = pl.BlockSpec(memory_space=pltpu.VMEM)
SMEM = pl.BlockSpec(memory_space=pltpu.SMEM)
HBM = pl.BlockSpec(memory_space=pltpu.HBM)
PARAMS = pltpu.CompilerParams(vmem_limit_bytes=8 * 1024 * 1024)
LANES, TILE, PAIRS = 128, 8, 5
F32, BF16 = jnp.float32, jnp.bfloat16


def accumulate(counts, grads, master, moment1, moment2, keep, give, shards, slots, acc, small, sems):
    _, n_slots, _, rows, width = grads.shape
    spans = 2 * keep.shape[0] // (TILE * rows)
    span, lines = width // spans, width // (spans * LANES)
    group = min(TILE, rows // 2)
    pieces = [(z, i) for z in range(spans) for i in range(0, rows // 2, group)]
    copies = []
    for n, (z, i) in enumerate(pieces):
        at = (pl.ds(2 * i, 2 * group), pl.ds(z * span, span))
        copies.append(pltpu.make_async_copy(grads.at[0, :, 0, *at], slots.at[:, *at], sems.at[n]))
    later = [
        pltpu.make_async_copy(x.at[0], small.at[i], sems.at[len(pieces) + i]) for i, x in enumerate((master, moment1, moment2))
    ]
    for copy in copies + later:
        copy.start()
    core = lax.axis_index("core")
    count = counts[0]
    weights = [(slot < count).astype(F32) for slot in range(n_slots)]
    for n, (z, i) in enumerate(pieces):
        copies[n].wait()
        at = (slice(2 * i, 2 * (i + group)), slice(z * span, (z + 1) * span))
        total = slots[0, *at].astype(F32)
        for slot in range(1, n_slots):
            total = total + weights[slot] * slots[slot, *at].astype(F32)
        for k in range(lines):
            acc[n * lines + k] = total[:, k * LANES : (k + 1) * LANES]
        for k in range(lines):
            to = pl.ds((i * spans + z) * TILE + k, group, stride=spans * TILE)
            keep[to, :] = acc[n * lines + k, pl.ds(core, group, stride=2), :]
            give[to, :] = acc[n * lines + k, pl.ds(1 - core, group, stride=2), :]
    for copy in later:
        copy.wait()
    w = small.shape[-1]
    shards[...] = jnp.zeros(shards.shape, F32)
    shards[0, :, :w] = small[0]
    shards[0, :, w : 2 * w] = small[1]
    shards[1, 0:1, :w] = small[2, 0:1]
    shards[1, 0:1, w : 2 * w] = small[2, 1:2]


def add(tokens, x, y, shards, out, state):
    out[...] = x[...] + y[...]
    state[...] = shards[...]
    state[1, 0:1, LANES - 1 :] = jnp.full((1, 1), tokens[0].astype(F32))


def reduce_and_pack(parts, state, out):
    total = parts[0:TILE, :]
    for j in range(TILE, parts.shape[0], TILE):
        total = total + parts[j : j + TILE, :]
    for j in range(0, out.shape[0], PAIRS):
        for r in range(PAIRS - 1):
            out[j + r] = total[2 * r : 2 * r + 2, :]
        out[j + PAIRS - 2, 1:2, :] = state[1, 0:1, :]
        out[j + PAIRS - 1] = state[0]


def adam(parts, send, mine, summed, state, result):
    peers = parts.shape[0] // PAIRS
    _, _, block = send.shape
    w = block // peers
    for c in range(2):
        for r in range(-(-block // (2 * LANES))):
            first = c * peers // 2
            total = parts[first * PAIRS + r]
            for j in range(first + 1, first + peers // 2):
                total = total + parts[j * PAIRS + r]
            for k in range(2 * r, min(2 * r + 2, block // LANES)):
                summed[c : c + 1, k * LANES : (k + 1) * LANES] = total[k - 2 * r : k - 2 * r + 1, :]
    total = summed[...]
    for j in range(peers):
        at = slice(j * w, (j + 1) * w)
        pair = (j + 1) * PAIRS - 1
        state[0, :, at] = parts[pair, :, :w]
        state[1, :, at] = parts[pair, :, w : 2 * w]
        state[2, 0:1, at] = parts[pair - 1, 1:2, :w]
        state[2, 1:2, at] = parts[pair - 1, 1:2, w : 2 * w]
    master, moment1, moment2 = state[0], state[1], state[2]
    tokens = parts[PAIRS - 2, 1:2, LANES - 1 :]
    gradient = total / tokens
    first = 0.9 * moment1 + 0.1 * gradient
    second = 0.95 * moment2 + 0.05 * gradient * gradient
    first_fix = 1.0 - 0.9**10
    second_fix = 1.0 - 0.95**10
    update = first / first_fix / (jnp.sqrt(second / second_fix) + 1e-08)
    new_master = master - 0.01 * (update + 0.1 * master)
    params = new_master.astype(BF16)
    for j in range(send.shape[0]):
        send[j] = params
    result[0], result[1], result[2] = new_master, first, second
    place = lax.axis_index(LINE)
    for j in range(peers):

        @pl.when(place == j)
        def _():
            for i in range(3):
                mine[i] = result[i, :, j * w : (j + 1) * w]


def assemble(parts, mine, params, master_out, moment1_out, moment2_out, whole, sems):
    _, _, block = parts.shape
    rows, width = whole.shape
    spans = width // block
    outs = [pltpu.make_async_copy(mine.at[i], x.at[0], sems.at[i]) for i, x in enumerate((master_out, moment1_out, moment2_out))]
    for copy in outs:
        copy.start()
    for t in range(rows // 8):
        for i in range(4 * t, 4 * t + 4):
            for z in range(spans):
                whole[2 * i : 2 * i + 2, z * block : (z + 1) * block] = parts[i * spans + z]
        at = pl.ds(8 * t, 8)
        copy = pltpu.make_async_copy(whole.at[at], params.at[0, at], sems.at[3 + t])
        copy.start()
        outs.append(copy)
    for copy in outs:
        copy.wait()


def body(grads, counts, total_tokens, master, moment1, moment2):
    n_slots, _, rows, width = grads.shape[1:]
    n_plane, n_line = lax.axis_size(PLANE), lax.axis_size(LINE)
    block, w = rows * width // (2 * n_plane), master.shape[2]
    exchange = lambda x, axes: lax.all_to_all(x, axes, 0, 0, tiled=True)
    pinned = [pltpu.with_memory_space_constraint(x, pltpu.HBM) for x in (grads, master, moment1, moment2)]

    tiles = jax.ShapeDtypeStruct((n_plane * TILE, LANES), F32)
    pairs = jax.ShapeDtypeStruct((2, 2, LANES), F32)
    keep, give, shards = pl.pallas_call(
        accumulate,
        out_shape=(tiles, tiles, pairs),
        in_specs=[SMEM] + [HBM] * 4,
        out_specs=(VMEM,) * 3,
        scratch_shapes=[
            pltpu.VMEM((n_slots, rows, width), BF16),
            pltpu.VMEM((width // LANES * rows // 16, 16, LANES), F32),
            pltpu.VMEM((3, 2, w), F32),
            pltpu.SemaphoreType.DMA((width // block * rows // 16 + 3,)),
        ],
        compiler_params=PARAMS,
    )(counts, *pinned)
    given = lax.ppermute(give, "core", [(0, 1), (1, 0)])
    parts, state = pl.pallas_call(
        add,
        out_shape=(tiles, pairs),
        in_specs=[SMEM] + [VMEM] * 3,
        out_specs=(VMEM, VMEM),
        compiler_params=PARAMS,
    )(total_tokens, keep, given, shards)
    parts = exchange(parts, PLANE)
    packed = pl.pallas_call(
        reduce_and_pack,
        out_shape=jax.ShapeDtypeStruct((n_line * PAIRS, 2, LANES), F32),
        in_specs=[VMEM, VMEM],
        out_specs=VMEM,
        compiler_params=PARAMS,
    )(parts, state)
    packed = exchange(packed, LINE)
    send, mine = pl.pallas_call(
        adam,
        out_shape=(jax.ShapeDtypeStruct((n_plane, 2, block), BF16), jax.ShapeDtypeStruct((3, 2, w), F32)),
        in_specs=[VMEM],
        out_specs=(VMEM, VMEM),
        scratch_shapes=[pltpu.VMEM((2, block), F32), pltpu.VMEM((3, 2, block), F32), pltpu.VMEM((3, 2, block), F32)],
        compiler_params=PARAMS,
    )(packed)
    gathered = exchange(send, PLANE)
    shard = jax.ShapeDtypeStruct(master.shape, F32)
    return pl.pallas_call(
        assemble,
        out_shape=(jax.ShapeDtypeStruct((1, rows, width), BF16), shard, shard, shard),
        in_specs=[VMEM, VMEM],
        out_specs=(HBM,) * 4,
        scratch_shapes=[pltpu.VMEM((rows, width), BF16), pltpu.SemaphoreType.DMA((3 + rows // 8,))],
        compiler_params=PARAMS,
    )(gathered, mine)


def solution(mesh):
    gx, gy, gz = mesh.devices.shape
    fine = Mesh(mesh.devices.reshape(gx // 2, 2, gy, gz), ("zh", "core", "gy", "gz"))
    ranks = ("zh", "core", "gy", "gz")
    state = P(None, "gy", ("zh", "core", "gz"))
    return jax.shard_map(
        body,
        mesh=fine,
        in_specs=(P(ranks, None, None, None, None), P(ranks), P(), state, state, state),
        out_specs=(P(), state, state, state),
        check_vma=False,
    )
```

```python
import functools

import jax
import jax.numpy as jnp
from jax import lax
from jax.experimental import pallas as pl
from jax.experimental.pallas import tpu as pltpu
from jax.sharding import Mesh, PartitionSpec as P

PLANE = ("gy", "zh")
LINE = ("core", "gz")
VMEM = pl.BlockSpec(memory_space=pltpu.VMEM)
SMEM = pl.BlockSpec(memory_space=pltpu.SMEM)
HBM = pl.BlockSpec(memory_space=pltpu.HBM)
PARAMS = pltpu.CompilerParams(vmem_limit_bytes=8 * 1024 * 1024)
LANES, TILE, PAIRS = 128, 8, 5
F32, BF16 = jnp.float32, jnp.bfloat16


def accumulate(spans, counts, grads, master, moment1, moment2, keep, give, shards, slots, acc, small, sems):
    _, n_slots, _, rows, width = grads.shape
    span, lines = width // spans, width // (spans * LANES)
    group = min(TILE, rows // 2)
    pieces = [(z, i) for z in range(spans) for i in range(0, rows // 2, group)]
    copies = []
    for n, (z, i) in enumerate(pieces):
        at = (pl.ds(2 * i, 2 * group), pl.ds(z * span, span))
        copies.append(pltpu.make_async_copy(grads.at[0, :, 0, *at], slots.at[:, *at], sems.at[n]))
    later = [
        pltpu.make_async_copy(x.at[0], small.at[i], sems.at[len(pieces) + i]) for i, x in enumerate((master, moment1, moment2))
    ]
    for copy in copies + later:
        copy.start()
    core = lax.axis_index("core")
    count = counts[0]
    weights = [(slot < count).astype(F32) for slot in range(n_slots)]
    for n, (z, i) in enumerate(pieces):
        copies[n].wait()
        at = (slice(2 * i, 2 * (i + group)), slice(z * span, (z + 1) * span))
        total = slots[0, *at].astype(F32)
        for slot in range(1, n_slots):
            total = total + weights[slot] * slots[slot, *at].astype(F32)
        for k in range(lines):
            acc[n * lines + k] = total[:, k * LANES : (k + 1) * LANES]
        for k in range(lines):
            to = pl.ds((i * spans + z) * lines + k, group, stride=spans * lines)
            keep[to, :] = acc[n * lines + k, pl.ds(core, group, stride=2), :]
            give[to, :] = acc[n * lines + k, pl.ds(1 - core, group, stride=2), :]
    for copy in later:
        copy.wait()
    w = small.shape[-1]
    shards[...] = jnp.zeros(shards.shape, F32)
    shards[0, :, :w] = small[0]
    shards[0, :, w : 2 * w] = small[1]
    shards[1, 0:1, :w] = small[2, 0:1]
    shards[1, 0:1, w : 2 * w] = small[2, 1:2]


def add(tokens, x, y, shards, out, state):
    out[...] = x[...] + y[...]
    state[...] = shards[...]
    state[1, 0:1, LANES - 1 :] = jnp.full((1, 1), tokens[0].astype(F32))


def reduce_and_pack(lines, parts, state, out, summed):
    for k in range(lines):
        total = parts[pl.ds(k, TILE, stride=lines), :]
        for j in range(TILE * lines, parts.shape[0], TILE * lines):
            total = total + parts[pl.ds(j + k, TILE, stride=lines), :]
        summed[k : k + 1, :] = jnp.sum(total, axis=0, keepdims=True)
    total = summed[...]
    for j in range(0, out.shape[0], PAIRS):
        for r in range(PAIRS - 1):
            out[j + r] = total[2 * r : 2 * r + 2, :]
        out[j + PAIRS - 2, 1:2, :] = state[1, 0:1, :]
        out[j + PAIRS - 1] = state[0]


def adam(parts, send, mine, summed, state, result):
    peers = parts.shape[0] // PAIRS
    _, _, block = send.shape
    w = block // peers
    for c in range(2):
        for r in range(-(-block // (2 * LANES))):
            first = c * peers // 2
            total = parts[first * PAIRS + r]
            for j in range(first + 1, first + peers // 2):
                total = total + parts[j * PAIRS + r]
            for k in range(2 * r, min(2 * r + 2, block // LANES)):
                summed[c : c + 1, k * LANES : (k + 1) * LANES] = total[k - 2 * r : k - 2 * r + 1, :]
    total = summed[...]
    for j in range(peers):
        at = slice(j * w, (j + 1) * w)
        pair = (j + 1) * PAIRS - 1
        state[0, :, at] = parts[pair, :, :w]
        state[1, :, at] = parts[pair, :, w : 2 * w]
        state[2, 0:1, at] = parts[pair - 1, 1:2, :w]
        state[2, 1:2, at] = parts[pair - 1, 1:2, w : 2 * w]
    master, moment1, moment2 = state[0], state[1], state[2]
    tokens = parts[PAIRS - 2, 1:2, LANES - 1 :]
    gradient = total / tokens
    first = 0.9 * moment1 + 0.1 * gradient
    second = 0.95 * moment2 + 0.05 * gradient * gradient
    first_fix = 1.0 - 0.9**10
    second_fix = 1.0 - 0.95**10
    update = first / first_fix / (jnp.sqrt(second / second_fix) + 1e-08)
    new_master = master - 0.01 * (update + 0.1 * master)
    params = new_master.astype(BF16)
    for j in range(send.shape[0]):
        send[j] = params
    result[0], result[1], result[2] = new_master, first, second
    place = lax.axis_index(LINE)
    for j in range(peers):

        @pl.when(place == j)
        def _():
            for i in range(3):
                mine[i] = result[i, :, j * w : (j + 1) * w]


def assemble(parts, mine, params, master_out, moment1_out, moment2_out, whole, sems):
    _, _, block = parts.shape
    rows, width = whole.shape
    spans = width // block
    outs = [pltpu.make_async_copy(mine.at[i], x.at[0], sems.at[i]) for i, x in enumerate((master_out, moment1_out, moment2_out))]
    for copy in outs:
        copy.start()
    for t in range(rows // 8):
        for i in range(4 * t, 4 * t + 4):
            for z in range(spans):
                whole[2 * i : 2 * i + 2, z * block : (z + 1) * block] = parts[i * spans + z]
        at = pl.ds(8 * t, 8)
        copy = pltpu.make_async_copy(whole.at[at], params.at[0, at], sems.at[3 + t])
        copy.start()
        outs.append(copy)
    for copy in outs:
        copy.wait()


def body(grads, counts, total_tokens, master, moment1, moment2):
    n_slots, _, rows, width = grads.shape[1:]
    n_plane, n_line = lax.axis_size(PLANE), lax.axis_size(LINE)
    block, w = rows * width // (2 * n_plane), master.shape[2]
    exchange = lambda x, axes: lax.all_to_all(x, axes, 0, 0, tiled=True)
    pinned = [pltpu.with_memory_space_constraint(x, pltpu.HBM) for x in (grads, master, moment1, moment2)]

    tiles = jax.ShapeDtypeStruct((n_plane * block // LANES, LANES), F32)
    pairs = jax.ShapeDtypeStruct((2, 2, LANES), F32)
    keep, give, shards = pl.pallas_call(
        functools.partial(accumulate, width // block),
        out_shape=(tiles, tiles, pairs),
        in_specs=[SMEM] + [HBM] * 4,
        out_specs=(VMEM,) * 3,
        scratch_shapes=[
            pltpu.VMEM((n_slots, rows, width), BF16),
            pltpu.VMEM((width // LANES * rows // 16, 16, LANES), F32),
            pltpu.VMEM((3, 2, w), F32),
            pltpu.SemaphoreType.DMA((width // block * rows // 16 + 3,)),
        ],
        compiler_params=PARAMS,
    )(counts, *pinned)
    given = lax.ppermute(give, "core", [(0, 1), (1, 0)])
    parts, state = pl.pallas_call(
        add,
        out_shape=(tiles, pairs),
        in_specs=[SMEM] + [VMEM] * 3,
        out_specs=(VMEM, VMEM),
        compiler_params=PARAMS,
    )(total_tokens, keep, given, shards)
    parts = exchange(parts.reshape(-1, 1, LANES), PLANE).reshape(parts.shape)
    packed = pl.pallas_call(
        functools.partial(reduce_and_pack, block // LANES),
        out_shape=jax.ShapeDtypeStruct((n_line * PAIRS, 2, LANES), F32),
        in_specs=[VMEM, VMEM],
        out_specs=VMEM,
        scratch_shapes=[pltpu.VMEM((TILE, LANES), F32)],
        compiler_params=PARAMS,
    )(parts, state)
    packed = exchange(packed, LINE)
    send, mine = pl.pallas_call(
        adam,
        out_shape=(jax.ShapeDtypeStruct((n_plane, 2, block), BF16), jax.ShapeDtypeStruct((3, 2, w), F32)),
        in_specs=[VMEM],
        out_specs=(VMEM, VMEM),
        scratch_shapes=[pltpu.VMEM((2, block), F32), pltpu.VMEM((3, 2, block), F32), pltpu.VMEM((3, 2, block), F32)],
        compiler_params=PARAMS,
    )(packed)
    gathered = exchange(send, PLANE)
    shard = jax.ShapeDtypeStruct(master.shape, F32)
    return pl.pallas_call(
        assemble,
        out_shape=(jax.ShapeDtypeStruct((1, rows, width), BF16), shard, shard, shard),
        in_specs=[VMEM, VMEM],
        out_specs=(HBM,) * 4,
        scratch_shapes=[pltpu.VMEM((rows, width), BF16), pltpu.SemaphoreType.DMA((3 + rows // 8,))],
        compiler_params=PARAMS,
    )(gathered, mine)


def solution(mesh):
    gx, gy, gz = mesh.devices.shape
    fine = Mesh(mesh.devices.reshape(gx // 2, 2, gy, gz), ("zh", "core", "gy", "gz"))
    ranks = ("zh", "core", "gy", "gz")
    state = P(None, "gy", ("zh", "core", "gz"))
    return jax.shard_map(
        body,
        mesh=fine,
        in_specs=(P(ranks, None, None, None, None), P(ranks), P(), state, state, state),
        out_specs=(P(), state, state, state),
        check_vma=False,
    )
```

```python
import functools

import jax
import jax.numpy as jnp
from jax import lax
from jax.experimental import pallas as pl
from jax.experimental.pallas import tpu as pltpu
from jax.sharding import Mesh, PartitionSpec as P

PLANE = ("gy", "zh")
LINE = ("core", "gz")
VMEM = pl.BlockSpec(memory_space=pltpu.VMEM)
SMEM = pl.BlockSpec(memory_space=pltpu.SMEM)
HBM = pl.BlockSpec(memory_space=pltpu.HBM)
PARAMS = pltpu.CompilerParams(vmem_limit_bytes=8 * 1024 * 1024)
LANES, TILE, PAIRS = 128, 8, 5
F32, BF16 = jnp.float32, jnp.bfloat16


def accumulate(spans, counts, grads, master, moment1, moment2, keep, give, shards, slots, acc, small, sems):
    _, n_slots, _, rows, width = grads.shape
    span, lines = width // spans, width // (spans * LANES)
    group = min(TILE, rows // 2)
    pieces = [(z, i) for z in range(spans) for i in range(0, rows // 2, group)]
    copies = []
    for n, (z, i) in enumerate(pieces):
        for h in range(2):
            at = (pl.ds(h * n_slots // 2, n_slots // 2), pl.ds(2 * i, 2 * group), pl.ds(z * span, span))
            copies.append(pltpu.make_async_copy(grads.at[0, at[0], 0, *at[1:]], slots.at[at], sems.at[2 * n + h]))
    later = [
        pltpu.make_async_copy(x.at[0], small.at[i], sems.at[2 * len(pieces) + i]) for i, x in enumerate((master, moment1, moment2))
    ]
    for copy in copies + later:
        copy.start()
    core = lax.axis_index("core")
    count = counts[0]
    weights = [(slot < count).astype(F32) for slot in range(n_slots)]
    for n, (z, i) in enumerate(pieces):
        copies[2 * n].wait()
        copies[2 * n + 1].wait()
        at = (slice(2 * i, 2 * (i + group)), slice(z * span, (z + 1) * span))
        total = slots[0, *at].astype(F32)
        for slot in range(1, n_slots):
            total = total + weights[slot] * slots[slot, *at].astype(F32)
        for k in range(lines):
            acc[n * lines + k] = total[:, k * LANES : (k + 1) * LANES]
        for k in range(lines):
            to = pl.ds((i * spans + z) * lines + k, group, stride=spans * lines)
            keep[to, :] = acc[n * lines + k, pl.ds(core, group, stride=2), :]
            give[to, :] = acc[n * lines + k, pl.ds(1 - core, group, stride=2), :]
    for copy in later:
        copy.wait()
    w = small.shape[-1]
    shards[...] = jnp.zeros(shards.shape, F32)
    shards[0, :, :w] = small[0]
    shards[0, :, w : 2 * w] = small[1]
    shards[1, 0:1, :w] = small[2, 0:1]
    shards[1, 0:1, w : 2 * w] = small[2, 1:2]


def yield_links(nanos):
    @pl.when(lax.axis_index("core") == 1)
    def _():
        pl.delay(nanos)


def add(tokens, x, y, shards, out, state):
    out[...] = x[...] + y[...]
    state[...] = shards[...]
    state[1, 0:1, LANES - 1 :] = jnp.full((1, 1), tokens[0].astype(F32))
    yield_links(600)


def reduce_and_pack(lines, parts, state, out, summed):
    for k in range(lines):
        total = parts[pl.ds(k, TILE, stride=lines), :]
        for j in range(TILE * lines, parts.shape[0], TILE * lines):
            total = total + parts[pl.ds(j + k, TILE, stride=lines), :]
        summed[k : k + 1, :] = jnp.sum(total, axis=0, keepdims=True)
    total = summed[...]
    for j in range(0, out.shape[0], PAIRS):
        for r in range(PAIRS - 1):
            out[j + r] = total[2 * r : 2 * r + 2, :]
        out[j + PAIRS - 2, 1:2, :] = state[1, 0:1, :]
        out[j + PAIRS - 1] = state[0]


def adam(parts, send, mine, summed, state, result):
    peers = parts.shape[0] // PAIRS
    _, _, block = send.shape
    w = block // peers
    for c in range(2):
        for r in range(-(-block // (2 * LANES))):
            first = c * peers // 2
            total = parts[first * PAIRS + r]
            for j in range(first + 1, first + peers // 2):
                total = total + parts[j * PAIRS + r]
            for k in range(2 * r, min(2 * r + 2, block // LANES)):
                summed[c : c + 1, k * LANES : (k + 1) * LANES] = total[k - 2 * r : k - 2 * r + 1, :]
    total = summed[...]
    for j in range(peers):
        at = slice(j * w, (j + 1) * w)
        pair = (j + 1) * PAIRS - 1
        state[0, :, at] = parts[pair, :, :w]
        state[1, :, at] = parts[pair, :, w : 2 * w]
        state[2, 0:1, at] = parts[pair - 1, 1:2, :w]
        state[2, 1:2, at] = parts[pair - 1, 1:2, w : 2 * w]
    master, moment1, moment2 = state[0], state[1], state[2]
    tokens = parts[PAIRS - 2, 1:2, LANES - 1 :]
    gradient = total / tokens
    first = 0.9 * moment1 + 0.1 * gradient
    second = 0.95 * moment2 + 0.05 * gradient * gradient
    first_fix = 1.0 - 0.9**10
    second_fix = 1.0 - 0.95**10
    update = first / first_fix / (jnp.sqrt(second / second_fix) + 1e-08)
    new_master = master - 0.01 * (update + 0.1 * master)
    params = new_master.astype(BF16)
    for j in range(send.shape[0]):
        send[j] = params
    result[0], result[1], result[2] = new_master, first, second
    place = lax.axis_index(LINE)
    for j in range(peers):

        @pl.when(place == j)
        def _():
            for i in range(3):
                mine[i] = result[i, :, j * w : (j + 1) * w]

    yield_links(900)


def assemble(parts, mine, params, master_out, moment1_out, moment2_out, whole, sems):
    _, _, block = parts.shape
    rows, width = whole.shape
    spans = width // block
    outs = [pltpu.make_async_copy(mine.at[i], x.at[0], sems.at[i]) for i, x in enumerate((master_out, moment1_out, moment2_out))]
    for copy in outs:
        copy.start()
    for t in range(rows // 8):
        for i in range(4 * t, 4 * t + 4):
            for z in range(spans):
                whole[2 * i : 2 * i + 2, z * block : (z + 1) * block] = parts[i * spans + z]
        at = pl.ds(8 * t, 8)
        copy = pltpu.make_async_copy(whole.at[at], params.at[0, at], sems.at[3 + t])
        copy.start()
        outs.append(copy)
    for copy in outs:
        copy.wait()


def body(grads, counts, total_tokens, master, moment1, moment2):
    n_slots, _, rows, width = grads.shape[1:]
    n_plane, n_line = lax.axis_size(PLANE), lax.axis_size(LINE)
    block, w = rows * width // (2 * n_plane), master.shape[2]
    exchange = lambda x, axes: lax.all_to_all(x, axes, 0, 0, tiled=True)
    pinned = [pltpu.with_memory_space_constraint(x, pltpu.HBM) for x in (grads, master, moment1, moment2)]

    tiles = jax.ShapeDtypeStruct((n_plane * block // LANES, LANES), F32)
    pairs = jax.ShapeDtypeStruct((2, 2, LANES), F32)
    keep, give, shards = pl.pallas_call(
        functools.partial(accumulate, width // block),
        out_shape=(tiles, tiles, pairs),
        in_specs=[SMEM] + [HBM] * 4,
        out_specs=(VMEM,) * 3,
        scratch_shapes=[
            pltpu.VMEM((n_slots, rows, width), BF16),
            pltpu.VMEM((width // LANES * rows // 16, 16, LANES), F32),
            pltpu.VMEM((3, 2, w), F32),
            pltpu.SemaphoreType.DMA((2 * (width // block * rows // 16) + 3,)),
        ],
        compiler_params=PARAMS,
    )(counts, *pinned)
    given = lax.ppermute(give, "core", [(0, 1), (1, 0)])
    parts, state = pl.pallas_call(
        add,
        out_shape=(tiles, pairs),
        in_specs=[SMEM] + [VMEM] * 3,
        out_specs=(VMEM, VMEM),
        compiler_params=PARAMS,
    )(total_tokens, keep, given, shards)
    parts = exchange(parts.reshape(-1, 1, LANES), PLANE).reshape(parts.shape)
    packed = pl.pallas_call(
        functools.partial(reduce_and_pack, block // LANES),
        out_shape=jax.ShapeDtypeStruct((n_line * PAIRS, 2, LANES), F32),
        in_specs=[VMEM, VMEM],
        out_specs=VMEM,
        scratch_shapes=[pltpu.VMEM((TILE, LANES), F32)],
        compiler_params=PARAMS,
    )(parts, state)
    packed = exchange(packed, LINE)
    send, mine = pl.pallas_call(
        adam,
        out_shape=(jax.ShapeDtypeStruct((n_plane, 2, block), BF16), jax.ShapeDtypeStruct((3, 2, w), F32)),
        in_specs=[VMEM],
        out_specs=(VMEM, VMEM),
        scratch_shapes=[pltpu.VMEM((2, block), F32), pltpu.VMEM((3, 2, block), F32), pltpu.VMEM((3, 2, block), F32)],
        compiler_params=PARAMS,
    )(packed)
    gathered = exchange(send, PLANE)
    shard = jax.ShapeDtypeStruct(master.shape, F32)
    return pl.pallas_call(
        assemble,
        out_shape=(jax.ShapeDtypeStruct((1, rows, width), BF16), shard, shard, shard),
        in_specs=[VMEM, VMEM],
        out_specs=(HBM,) * 4,
        scratch_shapes=[pltpu.VMEM((rows, width), BF16), pltpu.SemaphoreType.DMA((3 + rows // 8,))],
        compiler_params=PARAMS,
    )(gathered, mine)


def solution(mesh):
    gx, gy, gz = mesh.devices.shape
    fine = Mesh(mesh.devices.reshape(gx // 2, 2, gy, gz), ("zh", "core", "gy", "gz"))
    ranks = ("zh", "core", "gy", "gz")
    state = P(None, "gy", ("zh", "core", "gz"))
    return jax.shard_map(
        body,
        mesh=fine,
        in_specs=(P(ranks, None, None, None, None), P(ranks), P(), state, state, state),
        out_specs=(P(), state, state, state),
        check_vma=False,
    )
```

```python
import functools

import jax
import jax.numpy as jnp
from jax import lax
from jax.experimental import pallas as pl
from jax.experimental.pallas import tpu as pltpu
from jax.sharding import Mesh, PartitionSpec as P

PLANE = ("gy", "zh")
LINE = ("core", "gz")
VMEM = pl.BlockSpec(memory_space=pltpu.VMEM)
SMEM = pl.BlockSpec(memory_space=pltpu.SMEM)
HBM = pl.BlockSpec(memory_space=pltpu.HBM)
PARAMS = pltpu.CompilerParams(vmem_limit_bytes=8 * 1024 * 1024)
LANES, TILE, PAIRS = 128, 8, 5
F32, BF16 = jnp.float32, jnp.bfloat16


def accumulate(spans, counts, grads, master, moment1, moment2, keep, give, shards, slots, acc, small, sems):
    _, n_slots, _, rows, width = grads.shape
    span, lines = width // spans, width // (spans * LANES)
    group = min(TILE, rows // 2)
    pieces = [(z, i) for z in range(spans) for i in range(0, rows // 2, group)]
    copies = []
    for n, (z, i) in enumerate(pieces):
        at = (pl.ds(2 * i, 2 * group), pl.ds(z * span, span))
        copies.append(pltpu.make_async_copy(grads.at[0, :, 0, *at], slots.at[:, *at], sems.at[n]))
    later = [
        pltpu.make_async_copy(x.at[0], small.at[i], sems.at[len(pieces) + i]) for i, x in enumerate((master, moment1, moment2))
    ]
    for copy in copies + later:
        copy.start()
    core = lax.axis_index("core")
    count = counts[0]
    weights = [(slot < count).astype(F32) for slot in range(n_slots)]
    for n, (z, i) in enumerate(pieces):
        copies[n].wait()
        at = (slice(2 * i, 2 * (i + group)), slice(z * span, (z + 1) * span))
        total = slots[0, *at].astype(F32)
        for slot in range(1, n_slots):
            total = total + weights[slot] * slots[slot, *at].astype(F32)
        for k in range(lines):
            acc[n * lines + k, : 2 * group] = total[:, k * LANES : (k + 1) * LANES]
        for k in range(lines):
            to = pl.ds((i * spans + z) * lines + k, group, stride=spans * lines)
            keep[to, :] = acc[n * lines + k, pl.ds(core, group, stride=2), :]
            give[to, :] = acc[n * lines + k, pl.ds(1 - core, group, stride=2), :]
    for copy in later:
        copy.wait()
    w = small.shape[-1]
    shards[...] = jnp.zeros(shards.shape, F32)
    shards[0, :, :w] = small[0]
    shards[0, :, w : 2 * w] = small[1]
    shards[1, 0:1, :w] = small[2, 0:1]
    shards[1, 0:1, w : 2 * w] = small[2, 1:2]


def add(tokens, x, y, shards, out, state):
    out[...] = x[...] + y[...]
    state[...] = shards[...]
    state[1, 0:1, LANES - 1 :] = jnp.full((1, 1), tokens[0].astype(F32))


def reduce_and_pack(lines, parts, state, out, summed):
    for k in range(lines):
        total = parts[pl.ds(k, TILE, stride=lines), :]
        for j in range(TILE * lines, parts.shape[0], TILE * lines):
            total = total + parts[pl.ds(j + k, TILE, stride=lines), :]
        summed[k : k + 1, :] = jnp.sum(total, axis=0, keepdims=True)
    total = summed[...]
    for j in range(0, out.shape[0], PAIRS):
        for r in range(PAIRS - 1):
            out[j + r] = total[2 * r : 2 * r + 2, :]
        out[j + PAIRS - 2, 1:2, :] = state[1, 0:1, :]
        out[j + PAIRS - 1] = state[0]


def adam(parts, send, mine, summed, state, result):
    peers = parts.shape[0] // PAIRS
    _, _, block = send.shape
    w = block // peers
    for c in range(2):
        for r in range(-(-block // (2 * LANES))):
            first = c * peers // 2
            total = parts[first * PAIRS + r]
            for j in range(first + 1, first + peers // 2):
                total = total + parts[j * PAIRS + r]
            for k in range(2 * r, min(2 * r + 2, block // LANES)):
                summed[c : c + 1, k * LANES : (k + 1) * LANES] = total[k - 2 * r : k - 2 * r + 1, :]
    total = summed[...]
    for j in range(peers):
        at = slice(j * w, (j + 1) * w)
        pair = (j + 1) * PAIRS - 1
        state[0, :, at] = parts[pair, :, :w]
        state[1, :, at] = parts[pair, :, w : 2 * w]
        state[2, 0:1, at] = parts[pair - 1, 1:2, :w]
        state[2, 1:2, at] = parts[pair - 1, 1:2, w : 2 * w]
    master, moment1, moment2 = state[0], state[1], state[2]
    tokens = parts[PAIRS - 2, 1:2, LANES - 1 :]
    gradient = total / tokens
    first = 0.9 * moment1 + 0.1 * gradient
    second = 0.95 * moment2 + 0.05 * gradient * gradient
    first_fix = 1.0 - 0.9**10
    second_fix = 1.0 - 0.95**10
    update = first / first_fix / (jnp.sqrt(second / second_fix) + 1e-08)
    new_master = master - 0.01 * (update + 0.1 * master)
    params = new_master.astype(BF16)
    for j in range(send.shape[0]):
        send[j] = params
    result[0], result[1], result[2] = new_master, first, second
    place = lax.axis_index(LINE)
    for j in range(peers):

        @pl.when(place == j)
        def _():
            for i in range(3):
                mine[i] = result[i, :, j * w : (j + 1) * w]


def assemble(parts, mine, params, master_out, moment1_out, moment2_out, whole, sems):
    _, _, block = parts.shape
    rows, width = whole.shape
    spans = width // block
    outs = [pltpu.make_async_copy(mine.at[i], x.at[0], sems.at[i]) for i, x in enumerate((master_out, moment1_out, moment2_out))]
    for copy in outs:
        copy.start()
    for t in range(rows // 8):
        for i in range(4 * t, 4 * t + 4):
            for z in range(spans):
                whole[2 * i : 2 * i + 2, z * block : (z + 1) * block] = parts[i * spans + z]
        at = pl.ds(8 * t, 8)
        copy = pltpu.make_async_copy(whole.at[at], params.at[0, at], sems.at[3 + t])
        copy.start()
        outs.append(copy)
    for copy in outs:
        copy.wait()


def body(grads, counts, total_tokens, master, moment1, moment2):
    n_slots, _, rows, width = grads.shape[1:]
    n_plane, n_line = lax.axis_size(PLANE), lax.axis_size(LINE)
    block, w = rows * width // (2 * n_plane), master.shape[2]
    exchange = lambda x, axes: lax.all_to_all(x, axes, 0, 0, tiled=True)
    pinned = [pltpu.with_memory_space_constraint(x, pltpu.HBM) for x in (grads, master, moment1, moment2)]

    tiles = jax.ShapeDtypeStruct((n_plane * block // LANES, LANES), F32)
    pairs = jax.ShapeDtypeStruct((2, 2, LANES), F32)
    keep, give, shards = pl.pallas_call(
        functools.partial(accumulate, width // block),
        out_shape=(tiles, tiles, pairs),
        in_specs=[SMEM] + [HBM] * 4,
        out_specs=(VMEM,) * 3,
        scratch_shapes=[
            pltpu.VMEM((n_slots, rows, width), BF16),
            pltpu.VMEM((width // LANES * rows // 16, 24, LANES), F32),
            pltpu.VMEM((3, 2, w), F32),
            pltpu.SemaphoreType.DMA((width // block * rows // 16 + 3,)),
        ],
        compiler_params=PARAMS,
    )(counts, *pinned)
    given = lax.ppermute(give, "core", [(0, 1), (1, 0)])
    parts, state = pl.pallas_call(
        add,
        out_shape=(tiles, pairs),
        in_specs=[SMEM] + [VMEM] * 3,
        out_specs=(VMEM, VMEM),
        compiler_params=PARAMS,
    )(total_tokens, keep, given, shards)
    parts = exchange(parts.reshape(-1, 1, LANES), PLANE).reshape(parts.shape)
    packed = pl.pallas_call(
        functools.partial(reduce_and_pack, block // LANES),
        out_shape=jax.ShapeDtypeStruct((n_line * PAIRS, 2, LANES), F32),
        in_specs=[VMEM, VMEM],
        out_specs=VMEM,
        scratch_shapes=[pltpu.VMEM((TILE, LANES), F32)],
        compiler_params=PARAMS,
    )(parts, state)
    packed = exchange(packed, LINE)
    send, mine = pl.pallas_call(
        adam,
        out_shape=(jax.ShapeDtypeStruct((n_plane, 2, block), BF16), jax.ShapeDtypeStruct((3, 2, w), F32)),
        in_specs=[VMEM],
        out_specs=(VMEM, VMEM),
        scratch_shapes=[pltpu.VMEM((2, block), F32), pltpu.VMEM((3, 2, block), F32), pltpu.VMEM((3, 2, block), F32)],
        compiler_params=PARAMS,
    )(packed)
    gathered = exchange(send, PLANE)
    shard = jax.ShapeDtypeStruct(master.shape, F32)
    return pl.pallas_call(
        assemble,
        out_shape=(jax.ShapeDtypeStruct((1, rows, width), BF16), shard, shard, shard),
        in_specs=[VMEM, VMEM],
        out_specs=(HBM,) * 4,
        scratch_shapes=[pltpu.VMEM((rows, width), BF16), pltpu.SemaphoreType.DMA((3 + rows // 8,))],
        compiler_params=PARAMS,
    )(gathered, mine)


def solution(mesh):
    gx, gy, gz = mesh.devices.shape
    fine = Mesh(mesh.devices.reshape(gx // 2, 2, gy, gz), ("zh", "core", "gy", "gz"))
    ranks = ("zh", "core", "gy", "gz")
    state = P(None, "gy", ("zh", "core", "gz"))
    return jax.shard_map(
        body,
        mesh=fine,
        in_specs=(P(ranks, None, None, None, None), P(ranks), P(), state, state, state),
        out_specs=(P(), state, state, state),
        check_vma=False,
    )
```

```python
import functools

import jax
import jax.numpy as jnp
from jax import lax
from jax.experimental import pallas as pl
from jax.experimental.pallas import tpu as pltpu
from jax.sharding import Mesh, PartitionSpec as P

PLANE = ("gy", "zh")
LINE = ("core", "gz")
VMEM = pl.BlockSpec(memory_space=pltpu.VMEM)
SMEM = pl.BlockSpec(memory_space=pltpu.SMEM)
HBM = pl.BlockSpec(memory_space=pltpu.HBM)
PARAMS = pltpu.CompilerParams(vmem_limit_bytes=8 * 1024 * 1024)
LANES, TILE, PAIRS = 128, 8, 5
F32, BF16 = jnp.float32, jnp.bfloat16


def accumulate(spans, counts, grads, master, moment1, moment2, keep, give, shards, slots, acc, small, sems):
    _, n_slots, _, rows, width = grads.shape
    span, lines = width // spans, width // (spans * LANES)
    group = min(TILE, rows // 2)
    pieces = [(z, i) for z in range(spans) for i in range(0, rows // 2, group)]
    copies = []
    for n, (z, i) in enumerate(pieces):
        at = (pl.ds(2 * i, 2 * group), pl.ds(z * span, span))
        copies.append(pltpu.make_async_copy(grads.at[0, :, 0, *at], slots.at[:, *at], sems.at[n]))
    later = [
        pltpu.make_async_copy(x.at[0], small.at[i], sems.at[len(pieces) + i]) for i, x in enumerate((master, moment1, moment2))
    ]
    for copy in copies + later:
        copy.start()
    core = lax.axis_index("core")
    count = counts[0]
    weights = [(slot < count).astype(F32) for slot in range(n_slots)]
    for n, (z, i) in enumerate(pieces):
        copies[n].wait()
        at = (slice(2 * i, 2 * (i + group)), slice(z * span, (z + 1) * span))
        total = slots[0, *at].astype(F32)
        for slot in range(1, n_slots):
            total = total + weights[slot] * slots[slot, *at].astype(F32)
        for k in range(lines):
            acc[n * lines + k, : 2 * group] = total[:, k * LANES : (k + 1) * LANES]
        for k in range(lines):
            to = pl.ds((i * spans + z) * lines + k, group, stride=spans * lines)
            keep[to, :] = acc[n * lines + k, pl.ds(core, group, stride=2), :]
            give[to, :] = acc[n * lines + k, pl.ds(1 - core, group, stride=2), :]
    for copy in later:
        copy.wait()
    w = small.shape[-1]
    shards[...] = jnp.zeros(shards.shape, F32)
    shards[0, :, :w] = small[0]
    shards[0, :, w : 2 * w] = small[1]
    shards[1, 0:1, :w] = small[2, 0:1]
    shards[1, 0:1, w : 2 * w] = small[2, 1:2]


def add(tokens, x, y, shards, out, state):
    out[...] = x[...] + y[...]
    state[...] = shards[...]
    state[1, 0:1, LANES - 1 :] = jnp.full((1, 1), tokens[0].astype(F32))


def reduce_and_pack(lines, parts, state, out, summed):
    for k in range(lines):
        total = parts[pl.ds(k, TILE, stride=lines), :]
        for j in range(TILE * lines, parts.shape[0], TILE * lines):
            total = total + parts[pl.ds(j + k, TILE, stride=lines), :]
        summed[k : k + 1, :] = jnp.sum(total, axis=0, keepdims=True)
    total = summed[...]
    for j in range(0, out.shape[0], PAIRS):
        for r in range(PAIRS - 1):
            out[j + r] = total[2 * r : 2 * r + 2, :]
        out[j + PAIRS - 2, 1:2, :] = state[1, 0:1, :]
        out[j + PAIRS - 1] = state[0]


def adam(parts, send, mine, summed, state, result):
    peers = parts.shape[0] // PAIRS
    _, _, block = send.shape
    w = block // peers
    for c in range(2):
        for r in range(-(-block // (2 * LANES))):
            first = c * peers // 2
            total = parts[first * PAIRS + r]
            for j in range(first + 1, first + peers // 2):
                total = total + parts[j * PAIRS + r]
            for k in range(2 * r, min(2 * r + 2, block // LANES)):
                summed[c : c + 1, k * LANES : (k + 1) * LANES] = total[k - 2 * r : k - 2 * r + 1, :]
    total = summed[...]
    for j in range(peers):
        at = slice(j * w, (j + 1) * w)
        pair = (j + 1) * PAIRS - 1
        state[0, :, at] = parts[pair, :, :w]
        state[1, :, at] = parts[pair, :, w : 2 * w]
        state[2, 0:1, at] = parts[pair - 1, 1:2, :w]
        state[2, 1:2, at] = parts[pair - 1, 1:2, w : 2 * w]
    master, moment1, moment2 = state[0], state[1], state[2]
    tokens = parts[PAIRS - 2, 1:2, LANES - 1 :]
    gradient = total / tokens
    first = 0.9 * moment1 + 0.1 * gradient
    second = 0.95 * moment2 + 0.05 * gradient * gradient
    first_fix = 1.0 - 0.9**10
    second_fix = 1.0 - 0.95**10
    update = first / first_fix / (jnp.sqrt(second / second_fix) + 1e-08)
    new_master = master - 0.01 * (update + 0.1 * master)
    params = new_master.astype(BF16)
    for j in range(send.shape[0]):
        send[j] = params
    result[0], result[1], result[2] = new_master, first, second
    place = lax.axis_index(LINE)
    for j in range(peers):

        @pl.when(place == j)
        def _():
            for i in range(3):
                mine[i] = result[i, :, j * w : (j + 1) * w]


def assemble(parts, mine, params, master_out, moment1_out, moment2_out, sems):
    _, _, block = parts.shape
    rows, width = params.shape[1:]
    spans = width // block
    outs = [pltpu.make_async_copy(mine.at[i], x.at[0], sems.at[i]) for i, x in enumerate((master_out, moment1_out, moment2_out))]
    for copy in outs:
        copy.start()
    for i in range(rows // 2):
        for z in range(spans):
            at = (pl.ds(2 * i, 2), pl.ds(z * block, block))
            copy = pltpu.make_async_copy(parts.at[i * spans + z], params.at[0, *at], sems.at[3 + i * spans + z])
            copy.start()
            outs.append(copy)
    for copy in outs:
        copy.wait()


def body(grads, counts, total_tokens, master, moment1, moment2):
    n_slots, _, rows, width = grads.shape[1:]
    n_plane, n_line = lax.axis_size(PLANE), lax.axis_size(LINE)
    block, w = rows * width // (2 * n_plane), master.shape[2]
    exchange = lambda x, axes: lax.all_to_all(x, axes, 0, 0, tiled=True)
    pinned = [pltpu.with_memory_space_constraint(x, pltpu.HBM) for x in (grads, master, moment1, moment2)]

    tiles = jax.ShapeDtypeStruct((n_plane * block // LANES, LANES), F32)
    pairs = jax.ShapeDtypeStruct((2, 2, LANES), F32)
    keep, give, shards = pl.pallas_call(
        functools.partial(accumulate, width // block),
        out_shape=(tiles, tiles, pairs),
        in_specs=[SMEM] + [HBM] * 4,
        out_specs=(VMEM,) * 3,
        scratch_shapes=[
            pltpu.VMEM((n_slots, rows, width), BF16),
            pltpu.VMEM((width // LANES * rows // 16, 24, LANES), F32),
            pltpu.VMEM((3, 2, w), F32),
            pltpu.SemaphoreType.DMA((width // block * rows // 16 + 3,)),
        ],
        compiler_params=PARAMS,
    )(counts, *pinned)
    given = lax.ppermute(give, "core", [(0, 1), (1, 0)])
    parts, state = pl.pallas_call(
        add,
        out_shape=(tiles, pairs),
        in_specs=[SMEM] + [VMEM] * 3,
        out_specs=(VMEM, VMEM),
        compiler_params=PARAMS,
    )(total_tokens, keep, given, shards)
    parts = exchange(parts.reshape(-1, 1, LANES), PLANE).reshape(parts.shape)
    packed = pl.pallas_call(
        functools.partial(reduce_and_pack, block // LANES),
        out_shape=jax.ShapeDtypeStruct((n_line * PAIRS, 2, LANES), F32),
        in_specs=[VMEM, VMEM],
        out_specs=VMEM,
        scratch_shapes=[pltpu.VMEM((TILE, LANES), F32)],
        compiler_params=PARAMS,
    )(parts, state)
    packed = exchange(packed, LINE)
    send, mine = pl.pallas_call(
        adam,
        out_shape=(jax.ShapeDtypeStruct((n_plane, 2, block), BF16), jax.ShapeDtypeStruct((3, 2, w), F32)),
        in_specs=[VMEM],
        out_specs=(VMEM, VMEM),
        scratch_shapes=[pltpu.VMEM((2, block), F32), pltpu.VMEM((3, 2, block), F32), pltpu.VMEM((3, 2, block), F32)],
        compiler_params=PARAMS,
    )(packed)
    gathered = exchange(send, PLANE)
    shard = jax.ShapeDtypeStruct(master.shape, F32)
    return pl.pallas_call(
        assemble,
        out_shape=(jax.ShapeDtypeStruct((1, rows, width), BF16), shard, shard, shard),
        in_specs=[VMEM, VMEM],
        out_specs=(HBM,) * 4,
        scratch_shapes=[pltpu.SemaphoreType.DMA((3 + n_plane,))],
        compiler_params=PARAMS,
    )(gathered, mine)


def solution(mesh):
    gx, gy, gz = mesh.devices.shape
    fine = Mesh(mesh.devices.reshape(gx // 2, 2, gy, gz), ("zh", "core", "gy", "gz"))
    ranks = ("zh", "core", "gy", "gz")
    state = P(None, "gy", ("zh", "core", "gz"))
    return jax.shard_map(
        body,
        mesh=fine,
        in_specs=(P(ranks, None, None, None, None), P(ranks), P(), state, state, state),
        out_specs=(P(), state, state, state),
        check_vma=False,
    )
```

```python
import functools

import jax
import jax.numpy as jnp
from jax import lax
from jax.experimental import pallas as pl
from jax.experimental.pallas import tpu as pltpu
from jax.sharding import Mesh, PartitionSpec as P

PLANE = ("gy", "zh")
LINE = ("core", "gz")
VMEM = pl.BlockSpec(memory_space=pltpu.VMEM)
SMEM = pl.BlockSpec(memory_space=pltpu.SMEM)
HBM = pl.BlockSpec(memory_space=pltpu.HBM)
PARAMS = pltpu.CompilerParams(vmem_limit_bytes=8 * 1024 * 1024)
LANES, TILE, PAIRS = 128, 8, 5
F32, BF16 = jnp.float32, jnp.bfloat16


def accumulate(spans, counts, grads, master, moment1, moment2, keep, give, shards, slots, acc, small, sems):
    _, n_slots, _, rows, width = grads.shape
    span, lines = width // spans, width // (spans * LANES)
    group = min(TILE, rows // 2)
    pieces = [(z, i) for z in range(spans) for i in range(0, rows // 2, group)]
    copies = []
    for n, (z, i) in enumerate(pieces):
        at = (pl.ds(2 * i, 2 * group), pl.ds(z * span, span))
        copies.append(pltpu.make_async_copy(grads.at[0, :, 0, *at], slots.at[:, *at], sems.at[n]))
    later = [
        pltpu.make_async_copy(x.at[0], small.at[i], sems.at[len(pieces) + i]) for i, x in enumerate((master, moment1, moment2))
    ]
    for copy in later + copies:
        copy.start()
    core = lax.axis_index("core")
    count = counts[0]
    weights = [(slot < count).astype(F32) for slot in range(n_slots)]
    for n, (z, i) in enumerate(pieces):
        copies[n].wait()
        at = (slice(2 * i, 2 * (i + group)), slice(z * span, (z + 1) * span))
        total = slots[0, *at].astype(F32)
        for slot in range(1, n_slots):
            total = total + weights[slot] * slots[slot, *at].astype(F32)
        for k in range(lines):
            acc[n * lines + k, : 2 * group] = total[:, k * LANES : (k + 1) * LANES]
        for k in range(lines):
            to = pl.ds((i * spans + z) * lines + k, group, stride=spans * lines)
            keep[to, :] = acc[n * lines + k, pl.ds(core, group, stride=2), :]
            give[to, :] = acc[n * lines + k, pl.ds(1 - core, group, stride=2), :]
    for copy in later:
        copy.wait()
    w = small.shape[-1]
    shards[...] = jnp.zeros(shards.shape, F32)
    shards[0, :, :w] = small[0]
    shards[0, :, w : 2 * w] = small[1]
    shards[1, 0:1, :w] = small[2, 0:1]
    shards[1, 0:1, w : 2 * w] = small[2, 1:2]


def add(tokens, x, y, shards, out, state):
    out[...] = x[...] + y[...]
    state[...] = shards[...]
    state[1, 0:1, LANES - 1 :] = jnp.full((1, 1), tokens[0].astype(F32))


def reduce_and_pack(lines, parts, state, out, summed):
    for k in range(lines):
        total = parts[pl.ds(k, TILE, stride=lines), :]
        for j in range(TILE * lines, parts.shape[0], TILE * lines):
            total = total + parts[pl.ds(j + k, TILE, stride=lines), :]
        summed[k : k + 1, :] = jnp.sum(total, axis=0, keepdims=True)
    total = summed[...]
    for j in range(0, out.shape[0], PAIRS):
        for r in range(PAIRS - 1):
            out[j + r] = total[2 * r : 2 * r + 2, :]
        out[j + PAIRS - 2, 1:2, :] = state[1, 0:1, :]
        out[j + PAIRS - 1] = state[0]


def adam(parts, send, mine, summed, state, result):
    peers = parts.shape[0] // PAIRS
    _, _, block = send.shape
    w = block // peers
    for c in range(2):
        for r in range(-(-block // (2 * LANES))):
            first = c * peers // 2
            total = parts[first * PAIRS + r]
            for j in range(first + 1, first + peers // 2):
                total = total + parts[j * PAIRS + r]
            for k in range(2 * r, min(2 * r + 2, block // LANES)):
                summed[c : c + 1, k * LANES : (k + 1) * LANES] = total[k - 2 * r : k - 2 * r + 1, :]
    total = summed[...]
    for j in range(peers):
        at = slice(j * w, (j + 1) * w)
        pair = (j + 1) * PAIRS - 1
        state[0, :, at] = parts[pair, :, :w]
        state[1, :, at] = parts[pair, :, w : 2 * w]
        state[2, 0:1, at] = parts[pair - 1, 1:2, :w]
        state[2, 1:2, at] = parts[pair - 1, 1:2, w : 2 * w]
    master, moment1, moment2 = state[0], state[1], state[2]
    tokens = parts[PAIRS - 2, 1:2, LANES - 1 :]
    gradient = total / tokens
    first = 0.9 * moment1 + 0.1 * gradient
    second = 0.95 * moment2 + 0.05 * gradient * gradient
    first_fix = 1.0 - 0.9**10
    second_fix = 1.0 - 0.95**10
    update = first / first_fix / (jnp.sqrt(second / second_fix) + 1e-08)
    new_master = master - 0.01 * (update + 0.1 * master)
    params = new_master.astype(BF16)
    for j in range(send.shape[0]):
        send[j] = params
    result[0], result[1], result[2] = new_master, first, second
    place = lax.axis_index(LINE)
    for j in range(peers):

        @pl.when(place == j)
        def _():
            for i in range(3):
                mine[i] = result[i, :, j * w : (j + 1) * w]


def assemble(parts, mine, params, master_out, moment1_out, moment2_out, whole, sems):
    _, _, block = parts.shape
    rows, width = whole.shape
    spans = width // block
    outs = [pltpu.make_async_copy(mine.at[i], x.at[0], sems.at[i]) for i, x in enumerate((master_out, moment1_out, moment2_out))]
    for copy in outs:
        copy.start()
    for t in range(rows // 8):
        for i in range(4 * t, 4 * t + 4):
            for z in range(spans):
                whole[2 * i : 2 * i + 2, z * block : (z + 1) * block] = parts[i * spans + z]
        at = pl.ds(8 * t, 8)
        copy = pltpu.make_async_copy(whole.at[at], params.at[0, at], sems.at[3 + t])
        copy.start()
        outs.append(copy)
    for copy in outs:
        copy.wait()


def body(grads, counts, total_tokens, master, moment1, moment2):
    n_slots, _, rows, width = grads.shape[1:]
    n_plane, n_line = lax.axis_size(PLANE), lax.axis_size(LINE)
    block, w = rows * width // (2 * n_plane), master.shape[2]
    exchange = lambda x, axes: lax.all_to_all(x, axes, 0, 0, tiled=True)
    pinned = [pltpu.with_memory_space_constraint(x, pltpu.HBM) for x in (grads, master, moment1, moment2)]

    tiles = jax.ShapeDtypeStruct((n_plane * block // LANES, LANES), F32)
    pairs = jax.ShapeDtypeStruct((2, 2, LANES), F32)
    keep, give, shards = pl.pallas_call(
        functools.partial(accumulate, width // block),
        out_shape=(tiles, tiles, pairs),
        in_specs=[SMEM] + [HBM] * 4,
        out_specs=(VMEM,) * 3,
        scratch_shapes=[
            pltpu.VMEM((n_slots, rows, width), BF16),
            pltpu.VMEM((width // LANES * rows // 16, 24, LANES), F32),
            pltpu.VMEM((3, 2, w), F32),
            pltpu.SemaphoreType.DMA((width // block * rows // 16 + 3,)),
        ],
        compiler_params=PARAMS,
    )(counts, *pinned)
    given = lax.ppermute(give, "core", [(0, 1), (1, 0)])
    parts, state = pl.pallas_call(
        add,
        out_shape=(tiles, pairs),
        in_specs=[SMEM] + [VMEM] * 3,
        out_specs=(VMEM, VMEM),
        compiler_params=PARAMS,
    )(total_tokens, keep, given, shards)
    parts = exchange(parts.reshape(-1, 1, LANES), PLANE).reshape(parts.shape)
    packed = pl.pallas_call(
        functools.partial(reduce_and_pack, block // LANES),
        out_shape=jax.ShapeDtypeStruct((n_line * PAIRS, 2, LANES), F32),
        in_specs=[VMEM, VMEM],
        out_specs=VMEM,
        scratch_shapes=[pltpu.VMEM((TILE, LANES), F32)],
        compiler_params=PARAMS,
    )(parts, state)
    packed = exchange(packed, LINE)
    send, mine = pl.pallas_call(
        adam,
        out_shape=(jax.ShapeDtypeStruct((n_plane, 2, block), BF16), jax.ShapeDtypeStruct((3, 2, w), F32)),
        in_specs=[VMEM],
        out_specs=(VMEM, VMEM),
        scratch_shapes=[pltpu.VMEM((2, block), F32), pltpu.VMEM((3, 2, block), F32), pltpu.VMEM((3, 2, block), F32)],
        compiler_params=PARAMS,
    )(packed)
    gathered = exchange(send, PLANE)
    shard = jax.ShapeDtypeStruct(master.shape, F32)
    return pl.pallas_call(
        assemble,
        out_shape=(jax.ShapeDtypeStruct((1, rows, width), BF16), shard, shard, shard),
        in_specs=[VMEM, VMEM],
        out_specs=(HBM,) * 4,
        scratch_shapes=[pltpu.VMEM((rows, width), BF16), pltpu.SemaphoreType.DMA((3 + rows // 8,))],
        compiler_params=PARAMS,
    )(gathered, mine)


def solution(mesh):
    gx, gy, gz = mesh.devices.shape
    fine = Mesh(mesh.devices.reshape(gx // 2, 2, gy, gz), ("zh", "core", "gy", "gz"))
    ranks = ("zh", "core", "gy", "gz")
    state = P(None, "gy", ("zh", "core", "gz"))
    return jax.shard_map(
        body,
        mesh=fine,
        in_specs=(P(ranks, None, None, None, None), P(ranks), P(), state, state, state),
        out_specs=(P(), state, state, state),
        check_vma=False,
    )
```
